256 devices in a mesh: pgroup: 32 (over y, x, core), tile: 8 (over z).
Axes of the slice: x: 4, y: 4, z: 8, core: 2. Of those that a mesh axis runs over, the one named last changes fastest.
Arguments:
- images: float32 [512, 256, 2048], P(('pgroup', 'tile')), may hold values from -6 to 6
- beams: float32 [512, 256, 2048], P(('pgroup', 'tile')), may hold values from 0.2 to 1
- row_block: int32 [512], P(('pgroup', 'tile')), may hold values from 0 to 30, as said below
- col_block: int32 [512], P(('pgroup', 'tile')), may hold values from 0 to 16
- band: int32 [512, 2], P(('pgroup', 'tile')), may hold values from 0 to 3
- row_frac: float32 [512], P(('pgroup', 'tile')), may hold values from 0.05 to 0.95
- col_frac: float32 [512], P(('pgroup', 'tile')), may hold values from 0.05 to 0.95
Outputs:
- numer: float32 [4096, 4096], P('tile', 'pgroup')
- weight: float32 [4096, 4096], P('tile', 'pgroup')
- normalised: float32 [4096, 4096], P('tile', 'pgroup')
The draws below stay inside these ranges and needn't reach their ends.
Inputs may be any that keep to these rules, and one draw needn't show every extreme that they name: With t = (p // 2) mod 8, row_block[p] - 4 t lies in 0 to 2, and the largest value is taken in every draw.
All inputs are finite; a program needn't handle non-finite values.
Results may differ from the reference program's by a relative error of at most 0.00002.
Values sent between devices are 32-bit elements; how exact they have to be, the bound alone decides.
A program may use at most 128 MiB of HBM per device.

```python
import math
import jax
import jax.numpy as jnp
from jax import lax

W = 2048
IMG_ROWS = 256
IMG_BLOCKS = 2
PTS_DEV = 2
POINTINGS = 512
TILE_BLOCKS = 4
SKY_ROWS = 4096
SKY_COLS = 4096
HALO = 4
N_TILE = 8


def draw_row_block(key, part):
    pointing = jnp.arange(POINTINGS, dtype=jnp.int32)
    owner = pointing // PTS_DEV % N_TILE
    offset = jax.random.randint(key, (POINTINGS,), 0, TILE_BLOCKS - IMG_BLOCKS + 1, dtype=jnp.int32)
    offset = offset.at[0].set(TILE_BLOCKS - IMG_BLOCKS)
    return owner * TILE_BLOCKS + offset


def place_ends(array, own_key, low, high):
    index_at = [jax.random.randint(jax.random.fold_in(own_key, axis), (), 0, length) for axis, length in enumerate(array.shape)]
    widest = array.shape.index(max(array.shape))
    next_to = index_at[:widest] + [(index_at[widest] + 1) % array.shape[widest]] + index_at[widest + 1:]
    return array.at[tuple(index_at)].set(low).at[tuple(next_to)].set(high)


def level_of(own_key, shape, shards, least, largest):
    factor_of = 1.0
    for dim, blocks in shards:
        draws = jax.random.uniform(jax.random.fold_in(jax.random.fold_in(own_key, 6), dim), (blocks,), jnp.float32, least / len(shards), largest / len(shards))
        factor_of = factor_of * jnp.repeat(jnp.exp(draws), shape[dim] // blocks).reshape((-1,) + (1,) * (len(shape) - 1 - dim))
    return factor_of


def centred(rng, dims, width, reach, cuts=(), kind=jnp.bfloat16):
    level = level_of(rng, dims, cuts, -0.22, 0.18) if cuts else 1.0
    entries = jax.random.normal(rng, dims, jnp.float32) * width * level
    return jnp.minimum(jnp.maximum(entries, -reach), reach).astype(kind)


def setup_inputs(seed: int = 0) -> dict:
    key_list = jax.random.split(jax.random.key(seed), 8)
    return {
        "images": centred(key_list[0], (POINTINGS, IMG_ROWS, W), 1.0, 6.0, ((0, 256),), jnp.float32),
        "beams": jnp.clip(jnp.exp(math.log(1.0) - 1.609438 * jax.random.uniform(key_list[1], (POINTINGS, IMG_ROWS, W), jnp.float32) ** level_of(key_list[1], (POINTINGS, IMG_ROWS, W), ((0, 256),), -0.2, 0.2)), 0.2, 1.0),
        "row_block": draw_row_block(jax.random.fold_in(key_list[7], 71), 0),
        "col_block": place_ends(jax.random.randint(key_list[3], (POINTINGS,), 0, (SKY_COLS - W) // 128 + 1), jax.random.fold_in(key_list[3], 1), 0, ((SKY_COLS - W) // 128 + 1) - 1).astype(jnp.int32),
        "band": place_ends(jax.random.randint(key_list[4], (POINTINGS, IMG_BLOCKS), 0, HALO), jax.random.fold_in(key_list[4], 1), 0, HALO - 1).astype(jnp.int32),
        "row_frac": jnp.clip(0.05 + 0.9 * jax.random.uniform(key_list[5], (POINTINGS,), jnp.float32) ** level_of(key_list[5], (POINTINGS,), ((0, 256),), -0.2, 0.2), 0.05, 0.95),
        "col_frac": jnp.clip(0.05 + 0.9 * jax.random.uniform(key_list[6], (POINTINGS,), jnp.float32) ** level_of(key_list[6], (POINTINGS,), ((0, 256),), -0.2, 0.2), 0.05, 0.95),
    }


def contribution(image_block, beam_block, shift, row_f, col_f):
    stacked = jnp.stack([beam_block * image_block, beam_block * beam_block])
    moved = jnp.concatenate([jnp.zeros_like(stacked[:, :, :1]), stacked[:, :, :-1]], axis=2)
    banded = (1.0 - col_f) * stacked + col_f * moved
    empty = jnp.zeros((2, 128 + HALO, banded.shape[2]), jnp.float32)
    zero = jnp.int32(0)
    first = lax.dynamic_update_slice(empty, (1.0 - row_f) * banded, (zero, shift.astype(jnp.int32), zero))
    second = lax.dynamic_update_slice(empty, row_f * banded, (zero, (shift + 1).astype(jnp.int32), zero))
    return first + second


def reference(images, beams, row_block, col_block, band, row_frac, col_frac):
    canvas = jnp.zeros((2, SKY_ROWS + 128 + HALO, SKY_COLS), jnp.float32)

    def visit(index, canvas):
        for block in range(IMG_BLOCKS):
            image_block = lax.dynamic_slice_in_dim(images[index], block * 128, 128, 0)
            beam_block = lax.dynamic_slice_in_dim(beams[index], block * 128, 128, 0)
            piece = contribution(image_block, beam_block, band[index, block], row_frac[index], col_frac[index])
            row_start = ((row_block[index] + block) * 128).astype(jnp.int32)
            col_start = (col_block[index] * 128).astype(jnp.int32)
            zero = jnp.int32(0)
            old = lax.dynamic_slice(canvas, (zero, row_start, col_start), piece.shape)
            canvas = lax.dynamic_update_slice(canvas, old + piece, (zero, row_start, col_start))
        return canvas

    canvas = lax.fori_loop(0, POINTINGS, visit, canvas)
    numer = canvas[0, :SKY_ROWS]
    weight = canvas[1, :SKY_ROWS]
    normalised = numer / jnp.maximum(weight, 0.05)
    return numer, weight, normalised
```

```python
import jax
import jax.numpy as jnp
from jax import lax
from jax.experimental import pallas as pl
from jax.experimental.pallas import tpu as pltpu
from jax.sharding import PartitionSpec as P

MESH = pl.DeviceIdType.MESH
STRIPS = 16
ROWS = 64
CHUNKS = 8
SKY = 512
LAG = 1


def kernel(
    images, beams, row_block, col_block, band, row_frac, col_frac,
    numer, weight, normalised,
    inp, cols, ra, rb, rc, ta, tb, tc, canvas, hal, hin,
    got_a, got_b, got_c, got_d, got_e, out, their_row, their_col,
    in_sem, par_send, par_recv, strip_send, strip_recv, hal_send, hal_recv,
    send_sem, recv_sem, out_sem,
):
    me = lax.axis_index("pgroup")
    tile = lax.axis_index("tile")
    core = lax.rem(me, 2)
    x = lax.rem(lax.div(me, 2), 4)
    y = lax.div(me, 8)
    partner = me + 1 - 2 * core
    su, sv = 2 + 6 * core, 8 - 6 * core
    u = x + (y - x) * core
    v = y + (x - y) * core
    up = lax.rem(u + 1, 4) * su + v * sv + core
    um = lax.rem(u + 3, 4) * su + v * sv + core
    vp = u * su + lax.rem(v + 1, 4) * sv + core
    vm = u * su + lax.rem(v + 3, 4) * sv + core
    zp, zm = lax.rem(tile + 1, 8), lax.rem(tile + 7, 8)

    def load(p, b, q):
        rows = pl.ds(128 * b, 128)
        source = (images, beams)[q]
        return pltpu.make_async_copy(source.at[p, rows, :], inp.at[p, q, rows, :], in_sem.at[p, b, q])

    for b in range(2):
        for p in range(2):
            for q in range(2):
                load(p, b, q).start()

    barrier = pltpu.get_barrier_semaphore()
    for other in (partner, up, um, vp, vm):
        pl.semaphore_signal(barrier, inc=1, device_id={"pgroup": other, "tile": tile}, device_id_type=MESH)
    for other in (zp, zm):
        pl.semaphore_signal(barrier, inc=1, device_id={"pgroup": me, "tile": other}, device_id_type=MESH)

    def to(src, dst, ssem, rsem, pgroup, z=None):
        return pltpu.make_async_remote_copy(
            src_ref=src, dst_ref=dst, send_sem=ssem, recv_sem=rsem,
            device_id={"pgroup": pgroup, "tile": tile if z is None else z}, device_id_type=MESH,
        )

    edge = jnp.zeros((STRIPS, 8, 128), jnp.float32)
    for p in range(2):
        for b in range(2):
            for q in range(2):
                cols[p, b, q, :, pl.ds(0, 8), :] = edge
                cols[p, b, q, :, pl.ds(136, 8), :] = edge
    for p in range(4):
        ra[p, STRIPS] = jnp.zeros((128, 128), jnp.float32)
        rb[p, STRIPS] = jnp.zeros((128, 128), jnp.float32)
        rc[p, STRIPS] = jnp.zeros((8, 128), jnp.float32)

    @pl.when(tile == 0)
    def _():
        hin[...] = jnp.zeros(hin.shape, jnp.float32)

    pl.semaphore_wait(barrier, 7)

    params = [
        to(row_block, their_row, par_send.at[0], par_recv.at[0], partner),
        to(col_block, their_col, par_send.at[1], par_recv.at[1], partner),
    ]
    for copy in params:
        copy.start()

    first = lax.broadcasted_iota(jnp.int32, (8, 128), 1) == 0

    def band_columns(p, b):
        g = col_frac[p]
        load(p, b, 0).wait()
        load(p, b, 1).wait()

        def step(t, carry):
            rows = pl.ds(pl.multiple_of(128 * b + 8 * t, 8), 8)
            below = pl.ds(pl.multiple_of(8 * t + 8, 8), 8)
            before = [jnp.zeros((8, 128), jnp.float32)] * 2
            for k in range(STRIPS):
                lanes = pl.ds(128 * k, 128)
                beam = inp[p, 1, rows, lanes]
                for q in range(2):
                    value = beam * inp[p, core if q == 0 else 1 - core, rows, lanes]
                    rolled = pltpu.roll(value, 1, 1)
                    moved = jnp.where(first, before[q], rolled)
                    before[q] = rolled
                    cols[p, b, q, k, below, :] = (1.0 - g) * value + g * moved
            return carry

        lax.fori_loop(0, 16, step, 0)

    def mix(p, b, q, k, start, length):
        f = row_frac[p]
        s = band[p, b]
        near = cols[p, b, q, k, pl.ds(start + 8 - s, length), :]
        far = cols[p, b, q, k, pl.ds(start + 7 - s, length), :]
        return (1.0 - f) * near + f * far

    def band_rows_a(p):
        def step(k, carry):
            ta[p, k] = mix(p, 0, 1, k, 0, 128)
            ra[p, k] = mix(p, 0, 0, k, 0, 128)
            return carry

        lax.fori_loop(0, STRIPS, step, 0)

    def band_rows_b(p):
        def step(k, carry):
            for q, (mid, low) in ((1, (tb, tc)), (0, (rb, rc))):
                body = mix(p, 1, q, k, 0, 128)
                mid[p, k, pl.ds(0, 8), :] = body[0:8] + mix(p, 0, q, k, 128, 8)
                mid[p, k, pl.ds(8, 120), :] = body[8:128]
                low[p, k] = mix(p, 1, q, k, 128, 8)
            return carry

        lax.fori_loop(0, STRIPS, step, 0)

    def strips(p, n):
        mine, theirs = ((ta, ra), (tb, rb), (tc, rc))[n]
        return to(mine.at[p], theirs.at[2 + p, pl.ds(0, STRIPS)], strip_send.at[p, n], strip_recv.at[p, n], partner)

    for p in range(2):
        band_columns(p, 0)
        band_rows_a(p)
        strips(p, 0).start()
    for p in range(2):
        band_columns(p, 1)
        band_rows_b(p)
        strips(p, 1).start()
        strips(p, 2).start()

    for copy in params:
        copy.wait()
    offs = [row_block[p] - 4 * tile for p in range(2)] + [their_row[p] - 4 * tile for p in range(2)]
    shifts = [col_block[p] for p in range(2)] + [their_col[p] for p in range(2)]

    def column_of(rel, c):
        return lax.rem(u + rel, 4) * su + lax.rem(v + lax.div(c, 2), 4) * sv + lax.rem(c, 2)

    def generate(k, rel, early):
        turn = lax.rem(k + 1, CHUNKS)
        block = lax.div(turn, 2)
        half = pl.multiple_of(lax.rem(turn, 2) * ROWS, ROWS)
        start = lax.rem(turn, 2) == 0

        def step(c, carry):
            j = column_of(rel, c)
            total = None
            extra = None
            for p in range(4):
                k_in = j - shifts[p]
                inside = (k_in >= 0) & (k_in < STRIPS)
                ia = jnp.where(inside & (block == offs[p]), k_in, STRIPS)
                part = ra[p, ia, pl.ds(half, ROWS), :]
                total = part if total is None else total + part
                if not early:
                    ib = jnp.where(inside & (block == offs[p] + 1), k_in, STRIPS)
                    total = total + rb[p, ib, pl.ds(half, ROWS), :]
                    ic = jnp.where(inside & start & (block == offs[p] + 2), k_in, STRIPS)
                    tail = rc[p, ic]
                    extra = tail if extra is None else extra + tail
            if early:
                canvas[rel, k, c] = total
            else:
                canvas[rel, k, c, pl.ds(0, 8), :] = total[0:8] + extra
                canvas[rel, k, c, pl.ds(8, ROWS - 8), :] = total[8:ROWS]
            return carry

        lax.fori_loop(0, 8, step, 0)

    def border(k, rel):
        @pl.when(k == CHUNKS - 1)
        def _():
            canvas[rel, k, :, pl.ds(0, 8), :] = canvas[rel, k, :, pl.ds(0, 8), :] + hin[rel]

    def copy_a(k, d):
        return to(canvas.at[2, k, pl.ds(4 * d, 4)], got_a.at[d, k], send_sem.at[0, d, k], recv_sem.at[0, d, k], (up, um)[d])

    def copy_b(k, d):
        return to(canvas.at[1 + 2 * d, k], got_b.at[d, k], send_sem.at[1, d, k], recv_sem.at[1, d, k], (up, um)[d])

    def copy_c(k, d):
        return to(canvas.at[0, k, 4 + d], got_c.at[d, k], send_sem.at[2, d, k], recv_sem.at[2, d, k], (vp, vm)[d])

    def copy_d(k, d):
        return to(canvas.at[0, k, pl.ds(2 + 4 * d, 2)], got_d.at[d, k], send_sem.at[3, d, k], recv_sem.at[3, d, k], (vp, vm)[d])

    def copy_e(k):
        return to(canvas.at[0, k, 1 - core], got_e.at[k], send_sem.at[4, 0, k], recv_sem.at[4, 0, k], partner)

    def first_row(k):
        return pl.multiple_of(lax.rem(k + 1, CHUNKS) * ROWS, ROWS)

    def copy_out(k, n):
        rows = pl.ds(first_row(k), ROWS)
        return pltpu.make_async_copy(out.at[n, rows, :], (numer, weight, normalised)[n].at[rows, :], out_sem.at[n, k])

    strips(0, 0).wait_recv()
    strips(1, 0).wait_recv()
    generate(jnp.int32(0), 2, True)
    copy_a(0, 0).start()
    copy_a(0, 1).start()
    for rel in (1, 3, 0):
        generate(jnp.int32(0), rel, True)

    for n in (1, 2):
        for p in range(2):
            strips(p, n).wait_recv()

    halo = to(hal, hin, hal_send, hal_recv, me, zp)

    @pl.when(tile < 7)
    def _():
        def step(n, carry):
            j = column_of(lax.div(n, 8), lax.rem(n, 8))
            total = None
            for p in range(4):
                k_in = j - shifts[p]
                ic = jnp.where((k_in >= 0) & (k_in < STRIPS) & (offs[p] == 2), k_in, STRIPS)
                tail = rc[p, ic]
                total = tail if total is None else total + tail
            hal[lax.div(n, 8), lax.rem(n, 8)] = total
            return carry

        lax.fori_loop(0, 32, step, 0)
        halo.start()

    def iteration(i, carry):
        @pl.when(i < CHUNKS)
        def _():
            @pl.when((i == CHUNKS - 1) & (tile > 0))
            def _():
                halo.wait_recv()

            generate(i, 2, False)
            border(i, 2)
            copy_a(i, 0).start()
            copy_a(i, 1).start()
            for rel in (1, 3, 0):
                generate(i, rel, False)
                border(i, rel)

        kb = i - LAG

        @pl.when((kb >= 0) & (kb < CHUNKS))
        def _():
            for d in range(2):
                copy_a(kb, d).wait_recv()
                part = pl.ds(4 * d, 4)
                canvas[1 + 2 * d, kb, part] = canvas[1 + 2 * d, kb, part] + got_a[d, kb]
                copy_b(kb, d).start()

        kc = i - LAG - 1

        @pl.when((kc >= 0) & (kc < CHUNKS))
        def _():
            copy_b(kc, 0).wait_recv()
            copy_b(kc, 1).wait_recv()
            canvas[0, kc, pl.ds(4, 2)] = canvas[0, kc, pl.ds(4, 2)] + (got_b[0, kc, pl.ds(4, 2)] + got_b[1, kc, pl.ds(4, 2)])
            copy_c(kc, 0).start()
            copy_c(kc, 1).start()
            for part in (pl.ds(0, 4), pl.ds(6, 2)):
                canvas[0, kc, part] = canvas[0, kc, part] + (got_b[0, kc, part] + got_b[1, kc, part])

        kd = i - LAG - 2

        @pl.when((kd >= 0) & (kd < CHUNKS))
        def _():
            for d in range(2):
                copy_c(kd, d).wait_recv()
                spot = 2 + 5 * d
                canvas[0, kd, spot] = canvas[0, kd, spot] + got_c[d, kd]
                copy_d(kd, d).start()

        ke = i - LAG - 3

        @pl.when((ke >= 0) & (ke < CHUNKS))
        def _():
            copy_d(ke, 0).wait_recv()
            copy_d(ke, 1).wait_recv()
            canvas[0, ke, pl.ds(0, 2)] = canvas[0, ke, pl.ds(0, 2)] + (got_d[0, ke] + got_d[1, ke])
            copy_e(ke).start()

        kf = i - LAG - 4

        @pl.when(kf >= 0)
        def _():
            copy_e(kf).wait_recv()
            own = canvas[0, kf, core]
            got = got_e[kf]
            top = jnp.where(core == 0, own, got)
            low = jnp.where(core == 0, got, own)
            rows = pl.ds(first_row(kf), ROWS)
            out[0, rows, :] = top
            out[1, rows, :] = low
            out[2, rows, :] = top / jnp.maximum(low, 0.05)
            for n in range(3):
                copy_out(kf, n).start()

        return carry

    lax.fori_loop(1, CHUNKS + LAG + 4, iteration, 0)

    for copy in [strips(p, n) for p in range(2) for n in range(3)]:
        copy.wait_send()

    @pl.when(tile < 7)
    def _():
        halo.wait_send()

    def finish(k, carry):
        for d in range(2):
            for copy in (copy_a, copy_b, copy_c, copy_d):
                copy(k, d).wait_send()
        copy_e(k).wait_send()
        for n in range(3):
            copy_out(k, n).wait()
        return carry

    lax.fori_loop(0, CHUNKS, finish, 0)


def body(images, beams, row_block, col_block, band, row_frac, col_frac):
    f32 = jnp.float32
    vmem = lambda *shape: pltpu.VMEM(shape, f32)
    dma = pltpu.SemaphoreType.DMA
    piece = jax.ShapeDtypeStruct((SKY, 128), f32)
    hbm = pl.BlockSpec(memory_space=pl.ANY)
    smem = pl.BlockSpec(memory_space=pltpu.SMEM)
    return pl.pallas_call(
        kernel,
        out_shape=(piece, piece, piece),
        in_specs=[hbm, hbm, smem, smem, smem, smem, smem],
        out_specs=(hbm, hbm, hbm),
        scratch_shapes=[
            vmem(2, 2, 256, 2048),
            vmem(2, 2, 2, STRIPS, 144, 128),
            vmem(4, STRIPS + 1, 128, 128),
            vmem(4, STRIPS + 1, 128, 128),
            vmem(4, STRIPS + 1, 8, 128),
            vmem(2, STRIPS, 128, 128),
            vmem(2, STRIPS, 128, 128),
            vmem(2, STRIPS, 8, 128),
            vmem(4, CHUNKS, 8, ROWS, 128),
            vmem(4, 8, 8, 128),
            vmem(4, 8, 8, 128),
            vmem(2, CHUNKS, 4, ROWS, 128),
            vmem(2, CHUNKS, 8, ROWS, 128),
            vmem(2, CHUNKS, ROWS, 128),
            vmem(2, CHUNKS, 2, ROWS, 128),
            vmem(CHUNKS, ROWS, 128),
            vmem(3, SKY, 128),
            pltpu.SMEM((2,), jnp.int32),
            pltpu.SMEM((2,), jnp.int32),
            dma((2, 2, 2)),
            dma((2,)),
            dma((2,)),
            dma((2, 3)),
            dma((2, 3)),
            dma,
            dma,
            dma((5, 2, CHUNKS)),
            dma((5, 2, CHUNKS)),
            dma((3, CHUNKS)),
        ],
        compiler_params=pltpu.CompilerParams(
            collective_id=0, has_side_effects=True, vmem_limit_bytes=66_000_000
        ),
    )(images, beams, row_block, col_block, band, row_frac, col_frac)


def solution(mesh):
    return jax.shard_map(
        body,
        mesh=mesh,
        in_specs=(
            P(("pgroup", "tile"), None, None),
            P(("pgroup", "tile"), None, None),
            P(("pgroup", "tile")),
            P(("pgroup", "tile")),
            P(("pgroup", "tile"), None),
            P(("pgroup", "tile")),
            P(("pgroup", "tile")),
        ),
        out_specs=(P("tile", "pgroup"), P("tile", "pgroup"), P("tile", "pgroup")),
        check_vma=False,
    )
```

```python
import jax
import jax.numpy as jnp
from jax import lax
from jax.experimental import pallas as pl
from jax.experimental.pallas import tpu as pltpu
from jax.sharding import PartitionSpec as P

MESH = pl.DeviceIdType.MESH
STRIPS = 16
ROWS = 64
PARTS = 128 // ROWS
CHUNKS = 4 * PARTS
SKY = 512
SLOTS = 4
LAG_B, LAG_C, LAG_D, LAG_F = 1, 2, 3, 4


def kernel(
    images, beams, row_block, col_block, band, row_frac, col_frac,
    numer, weight, normalised,
    inp, cols, ra, rb, rc, ta, tb, tc, canvas, hal, hin,
    got_a, got_b, got_c, got_d, their_row, their_col,
    in_sem, par_send, par_recv, strip_send, strip_recv, hal_send, hal_recv,
    send_sem, recv_sem, last_recv,
):
    me = lax.axis_index("pgroup")
    tile = lax.axis_index("tile")
    core = lax.rem(me, 2)
    x = lax.rem(lax.div(me, 2), 4)
    y = lax.div(me, 8)
    partner = me + 1 - 2 * core
    su, sv = 2 + 6 * core, 8 - 6 * core
    u = x + (y - x) * core
    v = y + (x - y) * core
    up = lax.rem(u + 1, 4) * su + v * sv + core
    um = lax.rem(u + 3, 4) * su + v * sv + core
    vp = u * su + lax.rem(v + 1, 4) * sv + core
    vm = u * su + lax.rem(v + 3, 4) * sv + core
    zp, zm = lax.rem(tile + 1, 8), lax.rem(tile + 7, 8)

    barrier = pltpu.get_barrier_semaphore()
    for chip in (up - core, um - core, vp - core, vm - core):
        for other in (chip, chip + 1):
            pl.semaphore_signal(barrier, inc=1, device_id={"pgroup": other, "tile": tile}, device_id_type=MESH)
    pl.semaphore_signal(barrier, inc=1, device_id={"pgroup": partner, "tile": tile}, device_id_type=MESH)
    for other in (zp, zm):
        pl.semaphore_signal(barrier, inc=1, device_id={"pgroup": me, "tile": other}, device_id_type=MESH)

    def extent(h):
        return max(0, h * ROWS - 8), 128 if h == PARTS - 1 else (h + 1) * ROWS - 8

    def load(p, b, h, q):
        low, high = extent(h)
        rows = pl.ds(128 * b + low, high - low)
        source = (images, beams)[q]
        return pltpu.make_async_copy(source.at[p, rows, :], inp.at[p, q, rows, :], in_sem.at[p, b, h])

    def load_wait(p, b, h):
        low, high = extent(h)
        both = inp.at[p, :, pl.ds(128 * b + low, high - low), :]
        pltpu.make_async_copy(both, both, in_sem.at[p, b, h]).wait()

    def load_all(h, b):
        for p in range(2):
            for q in range(2):
                load(p, b, h, q).start()

    top = PARTS - 1
    load_all(top, 0)

    def to(src, dst, ssem, rsem, pgroup, z=None):
        return pltpu.make_async_remote_copy(
            src_ref=src, dst_ref=dst, send_sem=ssem, recv_sem=rsem,
            device_id={"pgroup": pgroup, "tile": tile if z is None else z}, device_id_type=MESH,
        )

    edge = jnp.zeros((STRIPS, 8, 128), jnp.float32)
    for p in range(2):
        for b in range(2):
            for q in range(2):
                cols[p, b, q, :, pl.ds(0, 8), :] = edge
                cols[p, b, q, :, pl.ds(136, 8), :] = edge
    for p in range(4):
        for h in range(PARTS):
            ra[h][p, STRIPS] = jnp.zeros((ROWS, 128), jnp.float32)
            rb[h][p, STRIPS] = jnp.zeros((ROWS, 128), jnp.float32)
        rc[p, STRIPS] = jnp.zeros((8, 128), jnp.float32)

    @pl.when(tile == 0)
    def _():
        hin[...] = jnp.zeros(hin.shape, jnp.float32)

    params = [
        to(row_block, their_row, par_send.at[0], par_recv.at[0], partner),
        to(col_block, their_col, par_send.at[1], par_recv.at[1], partner),
    ]
    first = lax.broadcasted_iota(jnp.int32, (8, 128), 1) == 0

    def band_columns(p, b, h):
        g = col_frac[p]
        load_wait(p, b, h)
        low, high = extent(h)
        for r in range(low, high, 8):
            rows = pl.ds(128 * b + r, 8)
            before = [jnp.zeros((8, 128), jnp.float32)] * 2
            for k in range(STRIPS):
                lanes = pl.ds(128 * k, 128)
                beam = inp[p, 1, rows, lanes]
                for q in range(2):
                    value = beam * inp[p, core if q == 0 else 1 - core, rows, lanes]
                    rolled = pltpu.roll(value, 1, 1)
                    moved = jnp.where(first, before[q], rolled)
                    before[q] = rolled
                    cols[p, b, q, k, pl.ds(r + 8, 8), :] = (1.0 - g) * value + g * moved

    def mix(p, b, q, k, start, length):
        f = row_frac[p]
        s = band[p, b]
        near = cols[p, b, q, k, pl.ds(start + 8 - s, length), :]
        far = cols[p, b, q, k, pl.ds(start + 7 - s, length), :]
        return (1.0 - f) * near + f * far

    def band_rows_a(p, h):
        def step(k, carry):
            ta[p, h, k] = mix(p, 0, 1, k, h * ROWS, ROWS)
            ra[h][p, k] = mix(p, 0, 0, k, h * ROWS, ROWS)
            return carry

        lax.fori_loop(0, STRIPS, step, 0)

    def band_rows_b(p, h):
        def step(k, carry):
            for q in (1, 0):
                part = mix(p, 1, q, k, h * ROWS, ROWS)
                spot = tb.at[p, h, k] if q else rb[h].at[p, k]
                if h == 0:
                    spot[pl.ds(0, 8), :] = part[0:8] + mix(p, 0, q, k, 128, 8)
                    spot[pl.ds(8, ROWS - 8), :] = part[8:ROWS]
                    low = tc if q else rc
                    low[p, k] = mix(p, 1, q, k, 128, 8)
                else:
                    spot[...] = part
            return carry

        lax.fori_loop(0, STRIPS, step, 0)

    def strips(p, n):
        kind, h = divmod(n, PARTS)
        mine = (ta.at[p, h], tb.at[p, h], tc.at[p])[kind]
        theirs = (ra[h], rb[h], rc)[kind]
        return to(mine, theirs.at[2 + p, pl.ds(0, STRIPS)], strip_send.at[n], strip_recv.at[n], partner)

    def strips_both(n):
        kind, h = divmod(n, PARTS)
        mine = (ta.at[:, h], tb.at[:, h], tc)[kind]
        theirs = (ra[h], rb[h], rc)[kind]
        return to(mine, theirs.at[pl.ds(2, 2), pl.ds(0, STRIPS)], strip_send.at[n], strip_recv.at[n], partner)

    for p in range(2):
        band_columns(p, 0, top)
        if p == 0:
            load_all(top, 1)
            for h in reversed(range(top)):
                load_all(h, 0)
                load_all(h, 1)
        band_rows_a(p, top)

    pl.semaphore_wait(barrier, 11)
    for copy in params:
        copy.start()
    for p in range(2):
        strips(p, top).start()
    for p in range(2):
        band_columns(p, 1, top)
        band_rows_b(p, top)
        strips(p, PARTS + top).start()

    for copy in params:
        copy.wait()
    offs = [row_block[p] - 4 * tile for p in range(2)] + [their_row[p] - 4 * tile for p in range(2)]
    shifts = [col_block[p] for p in range(2)] + [their_col[p] for p in range(2)]

    def column_of(rel, c):
        return lax.rem(u + rel, 4) * su + lax.rem(v + lax.div(c, 2), 4) * sv + lax.rem(c, 2)

    def block_of(k):
        return lax.rem(k + lax.div(k, CHUNKS - 4), 4)

    def generate(k, block, rel, h, early=False):
        def step(c, carry):
            j = column_of(rel, c)
            total = None
            extra = None
            for p in range(4):
                k_in = j - shifts[p]
                inside = (k_in >= 0) & (k_in < STRIPS)
                ia = jnp.where(inside & (block == offs[p]), k_in, STRIPS)
                part = ra[h][p, ia]
                total = part if total is None else total + part
                if not early:
                    ib = jnp.where(inside & (block == offs[p] + 1), k_in, STRIPS)
                    total = total + rb[h][p, ib]
                if h == 0:
                    ic = jnp.where(inside & (block == offs[p] + 2), k_in, STRIPS)
                    tail = rc[p, ic]
                    extra = tail if extra is None else extra + tail
            if h == 0:
                canvas[rel, k, c, pl.ds(0, 8), :] = total[0:8] + extra
                canvas[rel, k, c, pl.ds(8, ROWS - 8), :] = total[8:ROWS]
            else:
                canvas[rel, k, c] = total
            return carry

        lax.fori_loop(0, 8, step, 0)

        if h == 0:
            @pl.when(k == CHUNKS - 1)
            def _():
                canvas[rel, k, :, pl.ds(0, 8), :] = canvas[rel, k, :, pl.ds(0, 8), :] + hin[rel]

    def chunk(k):
        for h in range(PARTS):
            @pl.when(lax.div(k, 4) == PARTS - 1 - h)
            def _():
                block = block_of(k)
                generate(k, block, 2, h)
                send_a(k)
                for rel in (1, 3, 0):
                    generate(k, block, rel, h)

    def slot(k):
        return lax.rem(k, SLOTS)

    def copy_a(k, d):
        return to(canvas.at[2, k, pl.ds(4 * d, 4)], got_a.at[k, d], send_sem.at[0, slot(k)], recv_sem.at[0, slot(k)], (up, um)[d])

    def copy_b(k, d):
        return to(canvas.at[1 + 2 * d, k], got_b.at[k, d], send_sem.at[1, slot(k)], recv_sem.at[1, slot(k)], (up, um)[d])

    def copy_c(k, d):
        return to(canvas.at[0, k, 4 + d], got_c.at[k, d], send_sem.at[2, slot(k)], recv_sem.at[2, slot(k)], (vp, vm)[d])

    def copy_d(k, d, half):
        other = (vp, vm)[d] - core + half
        return to(canvas.at[0, k, 2 + 4 * d + half], got_d.at[k, 2 * core + d], send_sem.at[3, slot(k)], last_recv.at[k], other)

    def copy_e(k):
        return to(canvas.at[0, k, 1 - core], got_d.at[k, 4], send_sem.at[2, slot(k)], last_recv.at[k], partner)

    def await_recv(stage, k):
        if stage == 3:
            to(got_d.at[k], got_d.at[k], send_sem.at[3, 0], last_recv.at[k], partner).wait_recv()
        else:
            got = (got_a, got_b, got_c)[stage].at[k]
            to(got, got, send_sem.at[stage, 0], recv_sem.at[stage, slot(k)], partner).wait_recv()

    def await_send(stage, k):
        sent = (got_a.at[k], got_b.at[k], got_d.at[k, pl.ds(0, 3)], got_d.at[k, pl.ds(0, 4)])[stage]
        to(sent, sent, send_sem.at[stage, slot(k)], last_recv.at[0], partner).wait_send()

    def free(stage, k):
        @pl.when(k >= SLOTS)
        def _():
            await_send(stage, k - SLOTS)

    def send_a(k):
        copy_a(k, 0).start()
        copy_a(k, 1).start()

    def stage_b(k):
        await_recv(0, k)
        free(1, k)
        for d in range(2):
            part = pl.ds(4 * d, 4)
            canvas[1 + 2 * d, k, part] = canvas[1 + 2 * d, k, part] + got_a[k, d]
            copy_b(k, d).start()

    def stage_c(k):
        await_recv(1, k)
        free(2, k)
        for first_part, size in ((4, 2), (0, 4), (6, 2)):
            part = pl.ds(first_part, size)
            canvas[0, k, part] = canvas[0, k, part] + (got_b[k, 0, part] + got_b[k, 1, part])
            if first_part == 4:
                copy_c(k, 0).start()
                copy_c(k, 1).start()
        copy_e(k).start()

    def stage_d(k):
        await_recv(2, k)
        free(3, k)
        for d in range(2):
            spot = 2 + 5 * d
            canvas[0, k, spot] = canvas[0, k, spot] + got_c[k, d]
            copy_d(k, d, 0).start()
            copy_d(k, d, 1).start()

    def stage_f(k):
        await_recv(3, k)
        first_row = 128 * block_of(k) + ROWS * (PARTS - 1 - lax.div(k, 4))
        rows = pl.ds(pl.multiple_of(first_row, ROWS), ROWS)
        own = canvas[0, k, core] + (got_d[k, 2 * core] + got_d[k, 2 * core + 1])
        got = got_d[k, 4] + (got_d[k, 2 - 2 * core] + got_d[k, 3 - 2 * core])
        above = jnp.where(core == 0, own, got)
        below = jnp.where(core == 0, got, own)
        numer[rows, :] = above
        weight[rows, :] = below
        normalised[rows, :] = above / jnp.maximum(below, 0.05)

    strips_both(top).wait_recv()
    zero = jnp.int32(0)
    generate(zero, zero, 2, top, True)
    send_a(zero)
    for rel in (1, 3, 0):
        generate(zero, zero, rel, top, True)
    strips_both(PARTS + top).wait_recv()
    chunk_one = jnp.int32(1)
    generate(chunk_one, chunk_one, 2, top)
    send_a(chunk_one)
    for rel in (1, 3, 0):
        generate(chunk_one, chunk_one, rel, top)

    halo = to(hal, hin, hal_send, hal_recv, me, zp)

    def rest(h):
        for p in range(2):
            band_columns(p, 0, h)
            band_rows_a(p, h)
            strips(p, h).start()
            band_columns(p, 1, h)
            band_rows_b(p, h)
            strips(p, PARTS + h).start()
            if h == 0:
                strips(p, 2 * PARTS).start()

    def rest_wait(h):
        strips_both(h).wait_recv()
        strips_both(PARTS + h).wait_recv()
        if h == 0:
            strips_both(2 * PARTS).wait_recv()

    def send_halo():
        def step(n, carry):
            j = column_of(lax.div(n, 8), lax.rem(n, 8))
            total = None
            for p in range(4):
                k_in = j - shifts[p]
                ic = jnp.where((k_in >= 0) & (k_in < STRIPS) & (offs[p] == 2), k_in, STRIPS)
                tail = rc[p, ic]
                total = tail if total is None else total + tail
            hal[lax.div(n, 8), lax.rem(n, 8)] = total
            return carry

        lax.fori_loop(0, 32, step, 0)
        halo.start()

    def iteration(i, carry):
        for h in reversed(range(PARTS - 1)):
            k_first = 4 * (PARTS - 1 - h)

            @pl.when(i == k_first - 2)
            def _():
                rest(h)

            @pl.when(i == k_first)
            def _():
                rest_wait(h)
                if h == 0:
                    @pl.when(tile < 7)
                    def _():
                        send_halo()

        @pl.when((i == CHUNKS - 1) & (tile > 0))
        def _():
            halo.wait_recv()

        @pl.when(i < CHUNKS)
        def _():
            free(0, i)
            chunk(i)

        for lag, stage in ((LAG_B, stage_b), (LAG_D, stage_d), (LAG_F, stage_f), (LAG_C, stage_c)):
            @pl.when((i >= lag) & (i < CHUNKS + lag))
            def _():
                stage(i - lag)

        return carry

    if LAG_B == 1:
        stage_b(zero)
    lax.fori_loop(2, CHUNKS + LAG_F, iteration, 0)

    for stage in range(4):
        for k in range(CHUNKS - SLOTS, CHUNKS):
            await_send(stage, k)
    for n in range(2 * PARTS + 1):
        strips_both(n).wait_send()

    @pl.when(tile < 7)
    def _():
        halo.wait_send()


def store(numer, weight, normalised, numer_out, weight_out, normalised_out, sem):
    pairs = ((numer, numer_out), (weight, weight_out), (normalised, normalised_out))
    copies = [pltpu.make_async_copy(a, b, sem.at[n]) for n, (a, b) in enumerate(pairs)]
    for copy in copies:
        copy.start()
    for copy in copies:
        copy.wait()


def body(images, beams, row_block, col_block, band, row_frac, col_frac):
    f32 = jnp.float32
    vmem = lambda *shape: pltpu.VMEM(shape, f32)
    dma = pltpu.SemaphoreType.DMA
    piece = jax.ShapeDtypeStruct((SKY, 128), f32)
    hbm = pl.BlockSpec(memory_space=pl.ANY)
    smem = pl.BlockSpec(memory_space=pltpu.SMEM)
    local = pl.BlockSpec(memory_space=pltpu.VMEM)
    found = pl.pallas_call(
        kernel,
        out_shape=(pltpu.VMEM((SKY, 128), f32),) * 3,
        in_specs=[hbm, hbm, smem, smem, smem, smem, smem],
        out_specs=(local, local, local),
        scratch_shapes=[
            vmem(2, 2, 256, 2048),
            vmem(2, 2, 2, STRIPS, 144, 128),
            [vmem(4, STRIPS + 1, ROWS, 128) for _ in range(PARTS)],
            [vmem(4, STRIPS + 1, ROWS, 128) for _ in range(PARTS)],
            vmem(4, STRIPS + 1, 8, 128),
            vmem(2, PARTS, STRIPS, ROWS, 128),
            vmem(2, PARTS, STRIPS, ROWS, 128),
            vmem(2, STRIPS, 8, 128),
            vmem(4, CHUNKS, 8, ROWS, 128),
            vmem(4, 8, 8, 128),
            vmem(4, 8, 8, 128),
            vmem(CHUNKS, 2, 4, ROWS, 128),
            vmem(CHUNKS, 2, 8, ROWS, 128),
            vmem(CHUNKS, 2, ROWS, 128),
            vmem(CHUNKS, 5, ROWS, 128),
            pltpu.SMEM((2,), jnp.int32),
            pltpu.SMEM((2,), jnp.int32),
            dma((2, 2, PARTS)),
            dma((2,)),
            dma((2,)),
            dma((2 * PARTS + 1,)),
            dma((2 * PARTS + 1,)),
            dma,
            dma,
            dma((4, SLOTS)),
            dma((3, SLOTS)),
            dma((CHUNKS,)),
        ],
        compiler_params=pltpu.CompilerParams(
            collective_id=0, has_side_effects=True, vmem_limit_bytes=60_000_000
        ),
    )(images, beams, row_block, col_block, band, row_frac, col_frac)
    return pl.pallas_call(
        store,
        out_shape=(piece, piece, piece),
        in_specs=[local, local, local],
        out_specs=(hbm, hbm, hbm),
        scratch_shapes=[dma((3,))],
    )(*[pltpu.with_memory_space_constraint(a, pltpu.VMEM) for a in found])


def solution(mesh):
    return jax.shard_map(
        body,
        mesh=mesh,
        in_specs=(
            P(("pgroup", "tile"), None, None),
            P(("pgroup", "tile"), None, None),
            P(("pgroup", "tile")),
            P(("pgroup", "tile")),
            P(("pgroup", "tile"), None),
            P(("pgroup", "tile")),
            P(("pgroup", "tile")),
        ),
        out_specs=(P("tile", "pgroup"), P("tile", "pgroup"), P("tile", "pgroup")),
        check_vma=False,
    )
```

```python
import jax
import jax.numpy as jnp
from jax import lax
from jax.experimental import pallas as pl
from jax.experimental.pallas import tpu as pltpu
from jax.sharding import PartitionSpec as P

MESH = pl.DeviceIdType.MESH
STRIPS = 16
ROWS = 32
PARTS = 128 // ROWS
CHUNKS = 4 * PARTS
LAST = CHUNKS - 1
SKY = 512
SEND_SLOTS, RECV_SLOTS = 4, 8
LAG_B, LAG_C, LAG_D, LAG_F = 3, 6, 9, 12


def kernel(
    images, beams, row_block_in, col_block_in, band_in, row_frac_in, col_frac_in,
    numer, weight, normalised,
    inp, cols, ra, rb, rc, ta, tb, tc, canvas, hal, hin,
    got_a, got_b, got_c, got_d, row_block, col_block, band, row_frac, col_frac, their_row, their_col,
    in_sem, scalar_sem, par_send, par_recv, strip_send, strip_recv, hal_send, hal_recv,
    send_sem, recv_sem, last_recv, end_send,
):
    me = lax.axis_index("pgroup")
    tile = lax.axis_index("tile")
    core = lax.rem(me, 2)
    x = lax.rem(lax.div(me, 2), 4)
    y = lax.div(me, 8)
    partner = me + 1 - 2 * core
    su, sv = 2 + 6 * core, 8 - 6 * core
    u = x + (y - x) * core
    v = y + (x - y) * core
    up = lax.rem(u + 1, 4) * su + v * sv + core
    um = lax.rem(u + 3, 4) * su + v * sv + core
    vp = u * su + lax.rem(v + 1, 4) * sv + core
    vm = u * su + lax.rem(v + 3, 4) * sv + core
    uq = lax.rem(u + 2, 4) * su + v * sv + core
    vq = u * su + lax.rem(v + 2, 4) * sv + core

    def extent(h):
        return max(0, h * ROWS - 8), 128 if h == PARTS - 1 else (h + 1) * ROWS - 8

    def load(p, b, h, q):
        low, high = extent(h)
        rows = pl.ds(128 * b + low, high - low)
        source = (images, beams)[q]
        return pltpu.make_async_copy(source.at[p, rows, :], inp.at[p, q, rows, :], in_sem.at[p, b, h])

    def load_wait(p, b, h):
        low, high = extent(h)
        both = inp.at[p, :, pl.ds(128 * b + low, high - low), :]
        pltpu.make_async_copy(both, both, in_sem.at[p, b, h]).wait()

    def load_all(h, b):
        for p in range(2):
            for q in range(2):
                load(p, b, h, q).start()

    scalars = [
        pltpu.make_async_copy(src, dst, scalar_sem.at[n])
        for n, (src, dst) in enumerate((
            (col_frac_in, col_frac), (row_frac_in, row_frac), (band_in, band), (row_block_in, row_block), (col_block_in, col_block),
        ))
    ]

    top = PARTS - 1
    load_all(top, 0)
    for copy in scalars:
        copy.start()

    barrier = pltpu.get_barrier_semaphore()
    for chip in (up - core, um - core, vp - core, vm - core, uq - core, vq - core):
        for other in (chip, chip + 1):
            pl.semaphore_signal(barrier, inc=1, device_id={"pgroup": other, "tile": tile}, device_id_type=MESH)
    pl.semaphore_signal(barrier, inc=1, device_id={"pgroup": partner, "tile": tile}, device_id_type=MESH)
    for has, other in ((tile < 7, tile + 1), (tile > 0, tile - 1)):
        @pl.when(has)
        def _():
            pl.semaphore_signal(barrier, inc=1, device_id={"pgroup": me, "tile": other}, device_id_type=MESH)

    def to(src, dst, ssem, rsem, pgroup, z=None):
        return pltpu.make_async_remote_copy(
            src_ref=src, dst_ref=dst, send_sem=ssem, recv_sem=rsem,
            device_id={"pgroup": pgroup, "tile": tile if z is None else z}, device_id_type=MESH,
        )

    edge = jnp.zeros((STRIPS, 8, 128), jnp.float32)
    for p in range(2):
        for b in range(2):
            for q in range(2):
                cols[p, b, q, :, pl.ds(0, 8), :] = edge
                cols[p, b, q, :, pl.ds(136, 8), :] = edge
    for p in range(4):
        for h in range(PARTS):
            ra[h][p, STRIPS] = jnp.zeros((ROWS, 128), jnp.float32)
            rb[h][p, STRIPS] = jnp.zeros((ROWS, 128), jnp.float32)
        rc[p, STRIPS] = jnp.zeros((8, 128), jnp.float32)

    @pl.when(tile == 0)
    def _():
        hin[...] = jnp.zeros(hin.shape, jnp.float32)

    params = [
        to(row_block, their_row, par_send.at[0], par_recv.at[0], partner),
        to(col_block, their_col, par_send.at[1], par_recv.at[1], partner),
    ]
    first = lax.broadcasted_iota(jnp.int32, (8, 128), 1) == 0

    def band_columns(p, b, h):
        g = col_frac[p]
        load_wait(p, b, h)
        low, high = extent(h)
        for r in range(low, high, 8):
            rows = pl.ds(128 * b + r, 8)
            before = [jnp.zeros((8, 128), jnp.float32)] * 2
            for k in range(STRIPS):
                lanes = pl.ds(128 * k, 128)
                beam = inp[p, 1, rows, lanes]
                for q in range(2):
                    value = beam * inp[p, core if q == 0 else 1 - core, rows, lanes]
                    rolled = pltpu.roll(value, 1, 1)
                    moved = jnp.where(first, before[q], rolled)
                    before[q] = rolled
                    cols[p, b, q, k, pl.ds(r + 8, 8), :] = (1.0 - g) * value + g * moved

    def mix(p, b, q, k, start, length):
        f = row_frac[p]
        s = band[p, b]
        near = cols[p, b, q, k, pl.ds(start + 8 - s, length), :]
        far = cols[p, b, q, k, pl.ds(start + 7 - s, length), :]
        return (1.0 - f) * near + f * far

    def band_rows_a(p, h):
        def step(k, carry):
            ta[p, h, k] = mix(p, 0, 1, k, h * ROWS, ROWS)
            ra[h][p, k] = mix(p, 0, 0, k, h * ROWS, ROWS)
            return carry

        lax.fori_loop(0, STRIPS, step, 0)

    def band_rows_b(p, h):
        def step(k, carry):
            for q in (1, 0):
                part = mix(p, 1, q, k, h * ROWS, ROWS)
                spot = tb.at[p, h, k] if q else rb[h].at[p, k]
                if h == 0:
                    spot[pl.ds(0, 8), :] = part[0:8] + mix(p, 0, q, k, 128, 8)
                    spot[pl.ds(8, ROWS - 8), :] = part[8:ROWS]
                    low = tc if q else rc
                    low[p, k] = mix(p, 1, q, k, 128, 8)
                else:
                    spot[...] = part
            return carry

        lax.fori_loop(0, STRIPS, step, 0)

    def strips(p, n):
        kind, h = divmod(n, PARTS)
        mine = (ta.at[p, h], tb.at[p, h], tc.at[p])[kind]
        theirs = (ra[h], rb[h], rc)[kind]
        return to(mine, theirs.at[2 + p, pl.ds(0, STRIPS)], strip_send.at[n], strip_recv.at[n], partner)

    def strips_both(n):
        kind, h = divmod(n, PARTS)
        mine = (ta.at[:, h], tb.at[:, h], tc)[kind]
        theirs = (ra[h], rb[h], rc)[kind]
        return to(mine, theirs.at[pl.ds(2, 2), pl.ds(0, STRIPS)], strip_send.at[n], strip_recv.at[n], partner)

    for copy in scalars:
        copy.wait()
    for p in range(2):
        band_columns(p, 0, top)
        if p == 0:
            load_all(top, 1)
            for h in reversed(range(top)):
                load_all(h, 0)
                load_all(h, 1)
        band_rows_a(p, top)

    pl.semaphore_wait(barrier, 13 + jnp.where(tile < 7, 1, 0) + jnp.where(tile > 0, 1, 0))
    for copy in params:
        copy.start()
    for p in range(2):
        strips(p, top).start()
    for p in range(2):
        band_columns(p, 1, top)
        band_rows_b(p, top)
        strips(p, PARTS + top).start()

    for copy in params:
        copy.wait()
    offs = [row_block[p] - 4 * tile for p in range(2)] + [their_row[p] - 4 * tile for p in range(2)]
    shifts = [col_block[p] for p in range(2)] + [their_col[p] for p in range(2)]

    def column_of(rel, c):
        return lax.rem(u + rel, 4) * su + lax.rem(v + lax.div(c, 2), 4) * sv + lax.rem(c, 2)

    def block_of(k):
        return lax.rem(k + lax.div(k, CHUNKS - 4), 4)

    def generate(k, block, rel, h, early=False):
        def step(c, carry):
            j = column_of(rel, c)
            total = None
            extra = None
            for p in range(4):
                k_in = j - shifts[p]
                inside = (k_in >= 0) & (k_in < STRIPS)
                ia = jnp.where(inside & (block == offs[p]), k_in, STRIPS)
                part = ra[h][p, ia]
                total = part if total is None else total + part
                if not early:
                    ib = jnp.where(inside & (block == offs[p] + 1), k_in, STRIPS)
                    total = total + rb[h][p, ib]
                if h == 0:
                    ic = jnp.where(inside & (block == offs[p] + 2), k_in, STRIPS)
                    tail = rc[p, ic]
                    extra = tail if extra is None else extra + tail
            if h == 0:
                canvas[rel, k, c, pl.ds(0, 8), :] = total[0:8] + extra
                canvas[rel, k, c, pl.ds(8, ROWS - 8), :] = total[8:ROWS]
            else:
                canvas[rel, k, c] = total
            return carry

        lax.fori_loop(0, 8, step, 0)

        if h == 0:
            @pl.when(k == LAST)
            def _():
                canvas[rel, k, :, pl.ds(0, 8), :] = canvas[rel, k, :, pl.ds(0, 8), :] + hin[rel]

    def canvas_parts(k, rels):
        for h in range(PARTS):
            @pl.when(lax.div(k, 4) == PARTS - 1 - h)
            def _():
                for rel in rels:
                    generate(k, block_of(k), rel, h)

    def send_slot(k):
        return lax.rem(k, SEND_SLOTS)

    def slot(k):
        return lax.rem(k, RECV_SLOTS)

    def copy_a(k, d):
        return to(canvas.at[2, k, pl.ds(4 * d, 4)], got_a.at[k, d], send_sem.at[0, send_slot(k)], recv_sem.at[0, slot(k)], (up, um)[d])

    def copy_b(k, d):
        return to(canvas.at[1 + 2 * d, k], got_b.at[k, d], send_sem.at[1, send_slot(k)], recv_sem.at[1, slot(k)], (up, um)[d])

    def copy_c(k, d):
        return to(canvas.at[0, k, 4 + d], got_c.at[k, d], send_sem.at[2, send_slot(k)], recv_sem.at[2, slot(k)], (vp, vm)[d])

    def copy_d(k, d, half):
        other = (vp, vm)[d] - core + half
        return to(canvas.at[0, k, 2 + 4 * d + half], got_d.at[k, 2 * core + d], send_sem.at[3, send_slot(k)], last_recv.at[k], other)

    def copy_e(k):
        return to(canvas.at[0, k, 1 - core], got_d.at[k, 4], send_sem.at[2, send_slot(k)], last_recv.at[k], partner)

    def await_recv(stage, k):
        if stage >= 3:
            got = got_d.at[k, pl.ds(0, 5 if stage == 3 else 7)]
            to(got, got, send_sem.at[3, 0], last_recv.at[k], partner).wait_recv()
        else:
            got = (got_a, got_b, got_c)[stage].at[k]
            to(got, got, send_sem.at[stage, 0], recv_sem.at[stage, slot(k)], partner).wait_recv()

    def await_send(stage, k):
        sent = (got_a.at[k], got_b.at[k], got_d.at[k, pl.ds(0, 3)], got_d.at[k, pl.ds(0, 4)])[stage]
        to(sent, sent, send_sem.at[stage, send_slot(k)], last_recv.at[0], partner).wait_send()

    def free(stage, k):
        @pl.when(k >= SEND_SLOTS)
        def _():
            await_send(stage, k - SEND_SLOTS)

    def stage_a(k):
        free(0, k)
        canvas_parts(k, (2,))
        copy_a(k, 0).start()
        copy_a(k, 1).start()

    def stage_b(k):
        canvas_parts(k, (1, 3, 0))
        await_recv(0, k)
        free(1, k)
        for d in range(2):
            part = pl.ds(4 * d, 4)
            canvas[1 + 2 * d, k, part] = canvas[1 + 2 * d, k, part] + got_a[k, d]
            copy_b(k, d).start()

    def stage_c(k):
        await_recv(1, k)
        free(2, k)
        for first_part, size in ((4, 2), (0, 4), (6, 2)):
            part = pl.ds(first_part, size)
            canvas[0, k, part] = canvas[0, k, part] + (got_b[k, 0, part] + got_b[k, 1, part])
            if first_part == 4:
                copy_c(k, 0).start()
                copy_c(k, 1).start()
        copy_e(k).start()

    def stage_d(k):
        await_recv(2, k)
        free(3, k)
        for d in range(2):
            spot = 2 + 5 * d
            canvas[0, k, spot] = canvas[0, k, spot] + got_c[k, d]
            copy_d(k, d, 0).start()
            copy_d(k, d, 1).start()

    def copy_end(n, half):
        other = (vp, vm, vq)[n] - core + half
        piece = canvas.at[0, LAST, (2, 6, 4)[n] + half]
        return to(piece, got_d.at[LAST, (2 * core, 2 * core + 1, 5 + core)[n]], end_send, last_recv.at[LAST], other)

    def copy_end_own():
        return to(canvas.at[0, LAST, 1 - core], got_d.at[LAST, 4], end_send, last_recv.at[LAST], partner)

    def stage_end():
        await_recv(1, LAST)
        for n, first_part in ((2, 4), (0, 2), (1, 6)):
            part = pl.ds(first_part, 2)
            canvas[0, LAST, part] = canvas[0, LAST, part] + (got_b[LAST, 0, part] + got_b[LAST, 1, part])
            for half in range(2):
                copy_end(n, half).start()
        part = pl.ds(0, 2)
        canvas[0, LAST, part] = canvas[0, LAST, part] + (got_b[LAST, 0, part] + got_b[LAST, 1, part])
        copy_end_own().start()

    def stage_f(k, last=False):
        await_recv(4 if last else 3, k)
        first_row = 128 * block_of(k) + ROWS * (PARTS - 1 - lax.div(k, 4))
        rows = pl.ds(pl.multiple_of(first_row, ROWS), ROWS)
        own = canvas[0, k, core] + (got_d[k, 2 * core] + got_d[k, 2 * core + 1])
        got = got_d[k, 4] + (got_d[k, 2 - 2 * core] + got_d[k, 3 - 2 * core])
        if last:
            own = own + got_d[k, 5 + core]
            got = got + got_d[k, 6 - core]
        above = jnp.where(core == 0, own, got)
        below = jnp.where(core == 0, got, own)
        numer[rows, :] = above
        weight[rows, :] = below
        normalised[rows, :] = above / jnp.maximum(below, 0.05)

    halo = to(hal, hin, hal_send, hal_recv, me, lax.rem(tile + 1, 8))

    def rest(h, p):
        band_columns(p, 0, h)
        band_rows_a(p, h)
        strips(p, h).start()
        band_columns(p, 1, h)
        band_rows_b(p, h)
        strips(p, PARTS + h).start()
        if h == 0:
            strips(p, 2 * PARTS).start()

    def rest_wait(h):
        strips_both(h).wait_recv()
        strips_both(PARTS + h).wait_recv()
        if h == 0:
            strips_both(2 * PARTS).wait_recv()

    def send_halo():
        def step(n, carry):
            j = column_of(lax.div(n, 8), lax.rem(n, 8))
            total = None
            for p in range(4):
                k_in = j - shifts[p]
                ic = jnp.where((k_in >= 0) & (k_in < STRIPS) & (offs[p] == 2), k_in, STRIPS)
                tail = rc[p, ic]
                total = tail if total is None else total + tail
            hal[lax.div(n, 8), lax.rem(n, 8)] = total
            return carry

        lax.fori_loop(0, 32, step, 0)
        halo.start()

    def iteration(i, carry):
        for h in reversed(range(PARTS - 1)):
            @pl.when(i == part_start(h))
            def _():
                rest_wait(h)
                if h == 0:
                    @pl.when(tile < 7)
                    def _():
                        send_halo()

        @pl.when((i == LAST) & (tile > 0))
        def _():
            halo.wait_recv()

        @pl.when(i < CHUNKS)
        def _():
            stage_a(i)

        for h in reversed(range(PARTS - 1)):
            for p in range(2):
                if part_start(h) - 2 + p >= LAG_B:
                    @pl.when(i == part_start(h) - 2 + p)
                    def _():
                        rest(h, p)

        stages = ((LAG_B, stage_b, CHUNKS), (LAG_D, stage_d, LAST), (LAG_F, stage_f, LAST), (LAG_C, stage_c, LAST))
        for lag, stage, count in stages:
            @pl.when((i >= lag) & (i < count + lag))
            def _():
                stage(i - lag)

        @pl.when(i == LAST + LAG_C)
        def _():
            stage_end()

        return carry

    def part_start(h):
        return 4 * (PARTS - 1 - h)

    strips_both(top).wait_recv()
    generate(0, 0, 2, top, True)
    copy_a(0, 0).start()
    copy_a(0, 1).start()
    strips_both(PARTS + top).wait_recv()
    for i in range(1, LAG_B):
        generate(i, i, 2, top)
        copy_a(i, 0).start()
        copy_a(i, 1).start()
        for p in range(2):
            if i == part_start(top - 1) - 2 + p:
                rest(top - 1, p)
    lax.fori_loop(LAG_B, LAST + LAG_F, iteration, 0)
    stage_f(LAST, True)

    for stage in range(4):
        count = CHUNKS if stage < 2 else LAST
        for k in range(count - SEND_SLOTS, count):
            await_send(stage, k)
    to(got_d.at[LAST], got_d.at[LAST], end_send, last_recv.at[0], partner).wait_send()
    for n in range(2 * PARTS + 1):
        strips_both(n).wait_send()

    @pl.when(tile < 7)
    def _():
        halo.wait_send()


def store(numer, weight, normalised, numer_out, weight_out, normalised_out, sem):
    pairs = ((numer, numer_out), (weight, weight_out), (normalised, normalised_out))
    copies = [pltpu.make_async_copy(a, b, sem.at[n]) for n, (a, b) in enumerate(pairs)]
    for copy in copies:
        copy.start()
    for copy in copies:
        copy.wait()


def body(images, beams, row_block, col_block, band, row_frac, col_frac):
    f32 = jnp.float32
    vmem = lambda *shape: pltpu.VMEM(shape, f32)
    dma = pltpu.SemaphoreType.DMA
    piece = jax.ShapeDtypeStruct((SKY, 128), f32)
    hbm = pl.BlockSpec(memory_space=pl.ANY)
    local = pl.BlockSpec(memory_space=pltpu.VMEM)
    found = pl.pallas_call(
        kernel,
        out_shape=(pltpu.VMEM((SKY, 128), f32),) * 3,
        in_specs=[hbm] * 7,
        out_specs=(local, local, local),
        scratch_shapes=[
            vmem(2, 2, 256, 2048),
            vmem(2, 2, 2, STRIPS, 144, 128),
            [vmem(4, STRIPS + 1, ROWS, 128) for _ in range(PARTS)],
            [vmem(4, STRIPS + 1, ROWS, 128) for _ in range(PARTS)],
            vmem(4, STRIPS + 1, 8, 128),
            vmem(2, PARTS, STRIPS, ROWS, 128),
            vmem(2, PARTS, STRIPS, ROWS, 128),
            vmem(2, STRIPS, 8, 128),
            vmem(4, CHUNKS, 8, ROWS, 128),
            vmem(4, 8, 8, 128),
            vmem(4, 8, 8, 128),
            vmem(CHUNKS, 2, 4, ROWS, 128),
            vmem(CHUNKS, 2, 8, ROWS, 128),
            vmem(CHUNKS, 2, ROWS, 128),
            vmem(CHUNKS, 7, ROWS, 128),
            pltpu.SMEM((2,), jnp.int32),
            pltpu.SMEM((2,), jnp.int32),
            pltpu.SMEM((2, 2), jnp.int32),
            pltpu.SMEM((2,), f32),
            pltpu.SMEM((2,), f32),
            pltpu.SMEM((2,), jnp.int32),
            pltpu.SMEM((2,), jnp.int32),
            dma((2, 2, PARTS)),
            dma((5,)),
            dma((2,)),
            dma((2,)),
            dma((2 * PARTS + 1,)),
            dma((2 * PARTS + 1,)),
            dma,
            dma,
            dma((4, SEND_SLOTS)),
            dma((3, RECV_SLOTS)),
            dma((CHUNKS,)),
            dma,
        ],
        compiler_params=pltpu.CompilerParams(
            collective_id=0, has_side_effects=True, vmem_limit_bytes=60_000_000
        ),
    )(images, beams, row_block, col_block, band, row_frac, col_frac)
    return pl.pallas_call(
        store,
        out_shape=(piece, piece, piece),
        in_specs=[local, local, local],
        out_specs=(hbm, hbm, hbm),
        scratch_shapes=[dma((3,))],
    )(*[pltpu.with_memory_space_constraint(a, pltpu.VMEM) for a in found])


def solution(mesh):
    return jax.shard_map(
        body,
        mesh=mesh,
        in_specs=(
            P(("pgroup", "tile"), None, None),
            P(("pgroup", "tile"), None, None),
            P(("pgroup", "tile")),
            P(("pgroup", "tile")),
            P(("pgroup", "tile"), None),
            P(("pgroup", "tile")),
            P(("pgroup", "tile")),
        ),
        out_specs=(P("tile", "pgroup"), P("tile", "pgroup"), P("tile", "pgroup")),
        check_vma=False,
    )
```

```python
import jax
import jax.numpy as jnp
from jax import lax
from jax.experimental import pallas as pl
from jax.experimental.pallas import tpu as pltpu
from jax.sharding import PartitionSpec as P

MESH = pl.DeviceIdType.MESH
STRIPS = 16
ROWS = 32
PARTS = 128 // ROWS
CHUNKS = 4 * PARTS
LAST = CHUNKS - 1
UNROLL = 2
SKY = 512
SEND_SLOTS, RECV_SLOTS = (4, 4, 4, 4), (8, 8, 8)
LAG_B, LAG_C, LAG_D, LAG_F = 3, 6, 9, 12


def kernel(
    images, beams, row_block_in, col_block_in, band_in, row_frac_in, col_frac_in,
    numer, weight, normalised,
    inp, cols, ra, rb, rc, ta, tb, tc, canvas, hal, hin,
    got_a, got_b, got_c, got_d, row_block, col_block, band, row_frac, col_frac, their_row, their_col,
    in_sem, scalar_sem, par_send, par_recv, strip_send, strip_recv, hal_send, hal_recv,
    send_sem, recv_sem, last_recv, end_send,
):
    me = lax.axis_index("pgroup")
    tile = lax.axis_index("tile")
    core = lax.rem(me, 2)
    x = lax.rem(lax.div(me, 2), 4)
    y = lax.div(me, 8)
    partner = me + 1 - 2 * core
    su, sv = 2 + 6 * core, 8 - 6 * core
    u = x + (y - x) * core
    v = y + (x - y) * core
    up = lax.rem(u + 1, 4) * su + v * sv + core
    um = lax.rem(u + 3, 4) * su + v * sv + core
    vp = u * su + lax.rem(v + 1, 4) * sv + core
    vm = u * su + lax.rem(v + 3, 4) * sv + core
    vq = u * su + lax.rem(v + 2, 4) * sv + core

    def extent(h):
        return max(0, h * ROWS - 8), 128 if h == PARTS - 1 else (h + 1) * ROWS - 8

    top = PARTS - 1

    def load(p, b, h, q):
        low, high = extent(h)
        rows = pl.ds(128 * b + low, high - low)
        source = (images, beams)[q]
        return pltpu.make_async_copy(source.at[p, rows, :], inp.at[p, q, rows, :], in_sem.at[input_sem(p, b, h)])

    def input_sem(p, b, h):
        return 2 * PARTS if p == 1 and b == 0 and h == top else 2 * h + b

    def load_wait(p, b, h):
        low, high = extent(h)
        rows = pl.ds(128 * b + low, high - low)
        if b == 0 and h == top:
            part = inp.at[p, :, rows, :]
        elif p == 0:
            part = inp.at[:, :, rows, :]
        else:
            return
        pltpu.make_async_copy(part, part, in_sem.at[input_sem(p, b, h)]).wait()

    def load_all(h, b):
        for p in range(2):
            for q in range(2):
                load(p, b, h, q).start()

    scalars = [
        pltpu.make_async_copy(src, dst, scalar_sem.at[n])
        for n, (src, dst) in enumerate((
            (col_frac_in, col_frac), (row_frac_in, row_frac), (band_in, band), (row_block_in, row_block), (col_block_in, col_block),
        ))
    ]

    load_all(top, 0)
    for copy in scalars:
        copy.start()

    barrier = pltpu.get_barrier_semaphore()
    for chip in (up - core, um - core, vp - core, vm - core):
        for other in (chip, chip + 1):
            pl.semaphore_signal(barrier, inc=1, device_id={"pgroup": other, "tile": tile}, device_id_type=MESH)
    pl.semaphore_signal(barrier, inc=1, device_id={"pgroup": partner, "tile": tile}, device_id_type=MESH)
    for has, other in ((tile < 7, tile + 1), (tile > 0, tile - 1)):
        @pl.when(has)
        def _():
            pl.semaphore_signal(barrier, inc=1, device_id={"pgroup": me, "tile": other}, device_id_type=MESH)

    def to(src, dst, ssem, rsem, pgroup, z=None):
        return pltpu.make_async_remote_copy(
            src_ref=src, dst_ref=dst, send_sem=ssem, recv_sem=rsem,
            device_id={"pgroup": pgroup, "tile": tile if z is None else z}, device_id_type=MESH,
        )

    edge = jnp.zeros((STRIPS, 8, 128), jnp.float32)
    for p in range(2):
        for b in range(2):
            for q in range(2):
                cols[p, b, q, :, pl.ds(0, 8), :] = edge
                cols[p, b, q, :, pl.ds(136, 8), :] = edge
    for p in range(4):
        for h in range(PARTS):
            ra[h][p, STRIPS] = jnp.zeros((ROWS, 128), jnp.float32)
            rb[h][p, STRIPS] = jnp.zeros((ROWS, 128), jnp.float32)
        rc[p, STRIPS] = jnp.zeros((8, 128), jnp.float32)

    @pl.when(tile == 0)
    def _():
        hin[...] = jnp.zeros(hin.shape, jnp.float32)

    params = [
        to(row_block, their_row, par_send.at[0], par_recv.at[0], partner),
        to(col_block, their_col, par_send.at[1], par_recv.at[1], partner),
    ]
    first = lax.broadcasted_iota(jnp.int32, (8, 128), 1) == 0

    def band_columns(p, b, h):
        g = col_frac[p]
        load_wait(p, b, h)
        low, high = extent(h)
        for r in range(low, high, 8):
            rows = pl.ds(128 * b + r, 8)
            before = [jnp.zeros((8, 128), jnp.float32)] * 2
            for k in range(STRIPS):
                lanes = pl.ds(128 * k, 128)
                beam = inp[p, 1, rows, lanes]
                for q in range(2):
                    value = beam * inp[p, core if q == 0 else 1 - core, rows, lanes]
                    rolled = pltpu.roll(value, 1, 1)
                    moved = jnp.where(first, before[q], rolled)
                    before[q] = rolled
                    cols[p, b, q, k, pl.ds(r + 8, 8), :] = (1.0 - g) * value + g * moved

    def mix(p, b, q, k, start, length):
        f = row_frac[p]
        s = band[p, b]
        near = cols[p, b, q, k, pl.ds(start + 8 - s, length), :]
        far = cols[p, b, q, k, pl.ds(start + 7 - s, length), :]
        return (1.0 - f) * near + f * far

    def band_rows_a(p, h):
        def step(k, carry):
            ta[p, h, k] = mix(p, 0, 1, k, h * ROWS, ROWS)
            ra[h][p, k] = mix(p, 0, 0, k, h * ROWS, ROWS)
            return carry

        lax.fori_loop(0, STRIPS, step, 0)

    def band_rows_b(p, h):
        def step(k, carry):
            for q in (1, 0):
                part = mix(p, 1, q, k, h * ROWS, ROWS)
                spot = tb.at[p, h, k] if q else rb[h].at[p, k]
                if h == 0:
                    spot[pl.ds(0, 8), :] = part[0:8] + mix(p, 0, q, k, 128, 8)
                    spot[pl.ds(8, ROWS - 8), :] = part[8:ROWS]
                    low = tc if q else rc
                    low[p, k] = mix(p, 1, q, k, 128, 8)
                else:
                    spot[...] = part
            return carry

        lax.fori_loop(0, STRIPS, step, 0)

    def strips(p, n):
        kind, h = divmod(n, PARTS)
        mine = (ta.at[p, h], tb.at[p, h], tc.at[p])[kind]
        theirs = (ra[h], rb[h], rc)[kind]
        return to(mine, theirs.at[2 + p, pl.ds(0, STRIPS)], strip_send.at[n], strip_recv.at[n], partner)

    def strips_both(n):
        kind, h = divmod(n, PARTS)
        mine = (ta.at[:, h], tb.at[:, h], tc)[kind]
        theirs = (ra[h], rb[h], rc)[kind]
        return to(mine, theirs.at[pl.ds(2, 2), pl.ds(0, STRIPS)], strip_send.at[n], strip_recv.at[n], partner)

    for copy in scalars:
        copy.wait()
    for p in range(2):
        band_columns(p, 0, top)
        if p == 0:
            load_all(top, 1)
            for h in reversed(range(top)):
                load_all(h, 0)
                load_all(h, 1)
        band_rows_a(p, top)

    pl.semaphore_wait(barrier, 9 + jnp.where(tile < 7, 1, 0) + jnp.where(tile > 0, 1, 0))
    for copy in params:
        copy.start()
    for p in range(2):
        strips(p, top).start()
    for p in range(2):
        band_columns(p, 1, top)
        band_rows_b(p, top)
        strips(p, PARTS + top).start()

    for copy in params:
        copy.wait()
    offs = [row_block[p] - 4 * tile for p in range(2)] + [their_row[p] - 4 * tile for p in range(2)]
    shifts = [col_block[p] for p in range(2)] + [their_col[p] for p in range(2)]

    def column_of(rel, c):
        return lax.rem(u + rel, 4) * su + lax.rem(v + lax.div(c, 2), 4) * sv + lax.rem(c, 2)

    def block_of(k):
        return lax.rem(k + lax.div(k, CHUNKS - 4), 4)

    def generate(k, block, rel, h, early=False):
        reach = [
            [jnp.where(block == offs[p] + n, STRIPS, 0) for n in range(3)] for p in range(4)
        ]

        def pick(k_in, limit):
            return jnp.where((k_in >= 0) & (k_in < limit), k_in, STRIPS)

        def step(c, carry):
            for half in range(UNROLL):
                spot = UNROLL * c + half
                j = column_of(rel, spot)
                total = None
                extra = None
                for p in range(4):
                    k_in = j - shifts[p]
                    part = ra[h][p, pick(k_in, reach[p][0])]
                    total = part if total is None else total + part
                    if not early:
                        total = total + rb[h][p, pick(k_in, reach[p][1])]
                    if h == 0:
                        tail = rc[p, pick(k_in, reach[p][2])]
                        extra = tail if extra is None else extra + tail
                if h == 0:
                    canvas[rel, k, spot, pl.ds(0, 8), :] = total[0:8] + extra
                    canvas[rel, k, spot, pl.ds(8, ROWS - 8), :] = total[8:ROWS]
                else:
                    canvas[rel, k, spot] = total
            return carry

        lax.fori_loop(0, 8 // UNROLL, step, 0)

        if h == 0:
            @pl.when(k == LAST)
            def _():
                canvas[rel, k, :, pl.ds(0, 8), :] = canvas[rel, k, :, pl.ds(0, 8), :] + hin[rel]

    def canvas_parts(k, rels):
        for h in range(PARTS):
            @pl.when(lax.div(k, 4) == PARTS - 1 - h)
            def _():
                for rel in rels:
                    generate(k, block_of(k), rel, h)

    def sent(stage, k):
        return send_sem.at[sum(SEND_SLOTS[:stage]) + lax.rem(k, SEND_SLOTS[stage])]

    def landed(stage, k):
        return recv_sem.at[sum(RECV_SLOTS[:stage]) + lax.rem(k, RECV_SLOTS[stage])]

    def copy_a(k, d):
        return to(canvas.at[2, k, pl.ds(4 * d, 4)], got_a.at[k, d], sent(0, k), landed(0, k), (up, um)[d])

    def copy_b(k, d):
        return to(canvas.at[1 + 2 * d, k], got_b.at[k, d], sent(1, k), landed(1, k), (up, um)[d])

    def copy_c(k, d):
        return to(canvas.at[0, k, 4 + d], got_c.at[k, d], sent(2, k), landed(2, k), (vp, vm)[d])

    def copy_d(k, d, half):
        other = (vp, vm)[d] - core + half
        return to(canvas.at[0, k, 2 + 4 * d + half], got_d.at[k, 2 * core + d], sent(3, k), last_recv.at[k], other)

    def copy_e(k):
        return to(canvas.at[0, k, 1 - core], got_d.at[k, 4], sent(2, k), last_recv.at[k], partner)

    def await_recv(stage, k):
        if stage >= 3:
            got = got_d.at[k, pl.ds(0, 5 if stage == 3 else 7)]
            to(got, got, end_send, last_recv.at[k], partner).wait_recv()
        else:
            got = (got_a, got_b, got_c)[stage].at[k]
            to(got, got, end_send, landed(stage, k), partner).wait_recv()

    def await_send(stage, k):
        size = (got_a.at[k], got_b.at[k], got_d.at[k, pl.ds(0, 3)], got_d.at[k, pl.ds(0, 4)])[stage]
        to(size, size, sent(stage, k), last_recv.at[0], partner).wait_send()

    def free(stage, k):
        @pl.when(k >= SEND_SLOTS[stage])
        def _():
            await_send(stage, k - SEND_SLOTS[stage])

    def stage_a(k):
        free(0, k)
        canvas_parts(k, (2,))
        copy_a(k, 0).start()
        copy_a(k, 1).start()

    def stage_b(k):
        @pl.when(k > 0)
        def _():
            canvas_parts(k, (1, 3, 0))

        await_recv(0, k)
        free(1, k)
        for d in range(2):
            part = pl.ds(4 * d, 4)
            canvas[1 + 2 * d, k, part] = canvas[1 + 2 * d, k, part] + got_a[k, d]
            copy_b(k, d).start()

    def stage_c(k):
        await_recv(1, k)
        free(2, k)
        for first_part, size in ((4, 2), (0, 4), (6, 2)):
            part = pl.ds(first_part, size)
            canvas[0, k, part] = canvas[0, k, part] + (got_b[k, 0, part] + got_b[k, 1, part])
            if first_part == 4:
                copy_c(k, 0).start()
                copy_c(k, 1).start()
        copy_e(k).start()

    def stage_d(k):
        await_recv(2, k)
        free(3, k)
        for d in range(2):
            spot = 2 + 5 * d
            canvas[0, k, spot] = canvas[0, k, spot] + got_c[k, d]
            copy_d(k, d, 0).start()
            copy_d(k, d, 1).start()

    def copy_end(n, half):
        other = (vp, vm, vq)[n] - core + half
        piece = canvas.at[0, LAST, (2, 6, 4)[n] + half]
        return to(piece, got_d.at[LAST, (2 * core, 2 * core + 1, 5 + core)[n]], end_send, last_recv.at[LAST], other)

    def copy_end_own():
        return to(canvas.at[0, LAST, 1 - core], got_d.at[LAST, 4], end_send, last_recv.at[LAST], partner)

    def stage_end():
        await_recv(1, LAST)
        for n, first_part in ((2, 4), (0, 2), (1, 6)):
            part = pl.ds(first_part, 2)
            canvas[0, LAST, part] = canvas[0, LAST, part] + (got_b[LAST, 0, part] + got_b[LAST, 1, part])
            for half in range(2):
                copy_end(n, half).start()
        part = pl.ds(0, 2)
        canvas[0, LAST, part] = canvas[0, LAST, part] + (got_b[LAST, 0, part] + got_b[LAST, 1, part])
        copy_end_own().start()

    def stage_f(k, last=False):
        await_recv(4 if last else 3, k)
        first_row = 128 * block_of(k) + ROWS * (PARTS - 1 - lax.div(k, 4))
        rows = pl.ds(pl.multiple_of(first_row, ROWS), ROWS)
        own = canvas[0, k, core] + (got_d[k, 2 * core] + got_d[k, 2 * core + 1])
        got = got_d[k, 4] + (got_d[k, 2 - 2 * core] + got_d[k, 3 - 2 * core])
        if last:
            own = own + got_d[k, 5 + core]
            got = got + got_d[k, 6 - core]
        above = jnp.where(core == 0, own, got)
        below = jnp.where(core == 0, got, own)
        numer[rows, :] = above
        weight[rows, :] = below
        normalised[rows, :] = above / jnp.maximum(below, 0.05)

    halo = to(hal, hin, hal_send, hal_recv, me, lax.rem(tile + 1, 8))

    def rest(h, p):
        band_columns(p, 0, h)
        band_rows_a(p, h)
        strips(p, h).start()
        band_columns(p, 1, h)
        band_rows_b(p, h)
        strips(p, PARTS + h).start()
        if h == 0:
            strips(p, 2 * PARTS).start()

    def rest_wait(h):
        strips_both(h).wait_recv()
        strips_both(PARTS + h).wait_recv()
        if h == 0:
            strips_both(2 * PARTS).wait_recv()

    def send_halo():
        def step(n, carry):
            j = column_of(lax.div(n, 8), lax.rem(n, 8))
            total = None
            for p in range(4):
                k_in = j - shifts[p]
                ic = jnp.where((k_in >= 0) & (k_in < STRIPS) & (offs[p] == 2), k_in, STRIPS)
                tail = rc[p, ic]
                total = tail if total is None else total + tail
            hal[lax.div(n, 8), lax.rem(n, 8)] = total
            return carry

        lax.fori_loop(0, 32, step, 0)
        halo.start()

    def iteration(i, carry):
        for h in reversed(range(PARTS - 1)):
            @pl.when(i == part_start(h))
            def _():
                rest_wait(h)

        @pl.when((i == LAST) & (tile > 0))
        def _():
            halo.wait_recv()

        @pl.when(i < CHUNKS)
        def _():
            stage_a(i)

        for h in reversed(range(PARTS - 1)):
            for p in range(2):
                if rest_step(h, p) >= LAG_B:
                    @pl.when(i == rest_step(h, p))
                    def _():
                        rest(h, p)

        stages = ((LAG_B, stage_b, CHUNKS), (LAG_D, stage_d, LAST), (LAG_F, stage_f, LAST), (LAG_C, stage_c, LAST))
        for lag, stage, count in stages:
            @pl.when((i >= lag) & (i < count + lag))
            def _():
                stage(i - lag)

        @pl.when(i == LAST + LAG_C)
        def _():
            stage_end()

        @pl.when((i == part_start(0)) & (tile < 7))
        def _():
            send_halo()

        return carry

    def part_start(h):
        return 4 * (PARTS - 1 - h)

    def rest_step(h, p):
        return part_start(h) - (2 if h == top - 1 else 3) + p

    strips_both(top).wait_recv()
    generate(0, 0, 2, top, True)
    copy_a(0, 0).start()
    copy_a(0, 1).start()
    for rel in (1, 3, 0):
        generate(0, 0, rel, top, True)
    strips_both(PARTS + top).wait_recv()
    for i in range(1, LAG_B):
        generate(i, i, 2, top)
        copy_a(i, 0).start()
        copy_a(i, 1).start()
        for p in range(2):
            if i == rest_step(top - 1, p):
                rest(top - 1, p)
    lax.fori_loop(LAG_B, LAST + LAG_F, iteration, 0)
    stage_f(LAST, True)

    for stage in range(4):
        count = CHUNKS if stage < 2 else LAST
        for k in range(count - SEND_SLOTS[stage], count):
            await_send(stage, k)
    to(got_d.at[LAST], got_d.at[LAST], end_send, last_recv.at[0], partner).wait_send()
    for n in range(2 * PARTS + 1):
        strips_both(n).wait_send()

    @pl.when(tile < 7)
    def _():
        halo.wait_send()


def store(numer, weight, normalised, numer_out, weight_out, normalised_out, sem):
    pairs = ((numer, numer_out), (weight, weight_out), (normalised, normalised_out))
    copies = [pltpu.make_async_copy(a, b, sem.at[n]) for n, (a, b) in enumerate(pairs)]
    for copy in copies:
        copy.start()
    for copy in copies:
        copy.wait()


def body(images, beams, row_block, col_block, band, row_frac, col_frac):
    f32 = jnp.float32
    vmem = lambda *shape: pltpu.VMEM(shape, f32)
    dma = pltpu.SemaphoreType.DMA
    piece = jax.ShapeDtypeStruct((SKY, 128), f32)
    hbm = pl.BlockSpec(memory_space=pl.ANY)
    local = pl.BlockSpec(memory_space=pltpu.VMEM)
    found = pl.pallas_call(
        kernel,
        out_shape=(pltpu.VMEM((SKY, 128), f32),) * 3,
        in_specs=[hbm] * 7,
        out_specs=(local, local, local),
        scratch_shapes=[
            vmem(2, 2, 256, 2048),
            vmem(2, 2, 2, STRIPS, 144, 128),
            [vmem(4, STRIPS + 1, ROWS, 128) for _ in range(PARTS)],
            [vmem(4, STRIPS + 1, ROWS, 128) for _ in range(PARTS)],
            vmem(4, STRIPS + 1, 8, 128),
            vmem(2, PARTS, STRIPS, ROWS, 128),
            vmem(2, PARTS, STRIPS, ROWS, 128),
            vmem(2, STRIPS, 8, 128),
            vmem(4, CHUNKS, 8, ROWS, 128),
            vmem(4, 8, 8, 128),
            vmem(4, 8, 8, 128),
            vmem(CHUNKS, 2, 4, ROWS, 128),
            vmem(CHUNKS, 2, 8, ROWS, 128),
            vmem(CHUNKS, 2, ROWS, 128),
            vmem(CHUNKS, 7, ROWS, 128),
            pltpu.SMEM((2,), jnp.int32),
            pltpu.SMEM((2,), jnp.int32),
            pltpu.SMEM((2, 2), jnp.int32),
            pltpu.SMEM((2,), f32),
            pltpu.SMEM((2,), f32),
            pltpu.SMEM((2,), jnp.int32),
            pltpu.SMEM((2,), jnp.int32),
            dma((2 * PARTS + 1,)),
            dma((5,)),
            dma((2,)),
            dma((2,)),
            dma((2 * PARTS + 1,)),
            dma((2 * PARTS + 1,)),
            dma,
            dma,
            dma((sum(SEND_SLOTS),)),
            dma((sum(RECV_SLOTS),)),
            dma((CHUNKS,)),
            dma,
        ],
        compiler_params=pltpu.CompilerParams(
            collective_id=0, has_side_effects=True, vmem_limit_bytes=60_000_000
        ),
    )(images, beams, row_block, col_block, band, row_frac, col_frac)
    return pl.pallas_call(
        store,
        out_shape=(piece, piece, piece),
        in_specs=[local, local, local],
        out_specs=(hbm, hbm, hbm),
        scratch_shapes=[dma((3,))],
    )(*[pltpu.with_memory_space_constraint(a, pltpu.VMEM) for a in found])


def solution(mesh):
    return jax.shard_map(
        body,
        mesh=mesh,
        in_specs=(
            P(("pgroup", "tile"), None, None),
            P(("pgroup", "tile"), None, None),
            P(("pgroup", "tile")),
            P(("pgroup", "tile")),
            P(("pgroup", "tile"), None),
            P(("pgroup", "tile")),
            P(("pgroup", "tile")),
        ),
        out_specs=(P("tile", "pgroup"), P("tile", "pgroup"), P("tile", "pgroup")),
        check_vma=False,
    )
```

```python
import jax
import jax.numpy as jnp
from jax import lax
from jax.experimental import pallas as pl
from jax.experimental.pallas import tpu as pltpu
from jax.sharding import PartitionSpec as P

MESH = pl.DeviceIdType.MESH
STRIPS = 16
ROWS = 32
PARTS = 128 // ROWS
CHUNKS = 4 * PARTS
LAST = CHUNKS - 1
UNROLL = 2
SKY = 512
SEND_SLOTS, RECV_SLOTS = (4, 4, 4, 4), (8, 8, 8)
LAG_B, LAG_C, LAG_D, LAG_F = 3, 6, 8, 11


def kernel(
    images, beams, row_block_in, col_block_in, band_in, row_frac_in, col_frac_in,
    numer, weight, normalised,
    inp, cols, ra, rb, rc, ta, tb, tc, canvas, hal, hin,
    got_a, got_b, got_c, got_d, row_block, col_block, band, row_frac, col_frac, their_row, their_col,
    in_sem, scalar_sem, par_send, par_recv, strip_send, strip_recv, hal_send, hal_recv,
    send_sem, recv_sem, last_recv, end_send,
):
    me = lax.axis_index("pgroup")
    tile = lax.axis_index("tile")
    core = lax.rem(me, 2)
    x = lax.rem(lax.div(me, 2), 4)
    y = lax.div(me, 8)
    partner = me + 1 - 2 * core
    su, sv = 2 + 6 * core, 8 - 6 * core
    u = x + (y - x) * core
    v = y + (x - y) * core
    up = lax.rem(u + 1, 4) * su + v * sv + core
    um = lax.rem(u + 3, 4) * su + v * sv + core
    vp = u * su + lax.rem(v + 1, 4) * sv + core
    vm = u * su + lax.rem(v + 3, 4) * sv + core
    vq = u * su + lax.rem(v + 2, 4) * sv + core

    def extent(h):
        return max(0, h * ROWS - 8), 128 if h == PARTS - 1 else (h + 1) * ROWS - 8

    top = PARTS - 1

    def load(p, b, h, q):
        low, high = extent(h)
        rows = pl.ds(128 * b + low, high - low)
        source = (images, beams)[q]
        return pltpu.make_async_copy(source.at[p, rows, :], inp.at[p, q, rows, :], in_sem.at[input_sem(p, b, h)])

    def input_sem(p, b, h):
        return 2 * PARTS if p == 1 and b == 0 and h == top else 2 * h + b

    def load_wait(p, b, h):
        low, high = extent(h)
        rows = pl.ds(128 * b + low, high - low)
        if b == 0 and h == top:
            part = inp.at[p, :, rows, :]
        elif p == 0:
            part = inp.at[:, :, rows, :]
        else:
            return
        pltpu.make_async_copy(part, part, in_sem.at[input_sem(p, b, h)]).wait()

    def load_all(h, b):
        for p in range(2):
            for q in range(2):
                load(p, b, h, q).start()

    scalars = [
        pltpu.make_async_copy(src, dst, scalar_sem.at[n])
        for n, (src, dst) in enumerate((
            (col_frac_in, col_frac), (row_frac_in, row_frac), (band_in, band), (row_block_in, row_block), (col_block_in, col_block),
        ))
    ]

    load_all(top, 0)
    for copy in scalars:
        copy.start()

    barrier = pltpu.get_barrier_semaphore()
    for chip in (up - core, um - core, vp - core, vm - core):
        for other in (chip, chip + 1):
            pl.semaphore_signal(barrier, inc=1, device_id={"pgroup": other, "tile": tile}, device_id_type=MESH)
    pl.semaphore_signal(barrier, inc=1, device_id={"pgroup": partner, "tile": tile}, device_id_type=MESH)
    for has, other in ((tile < 7, tile + 1), (tile > 0, tile - 1)):
        @pl.when(has)
        def _():
            pl.semaphore_signal(barrier, inc=1, device_id={"pgroup": me, "tile": other}, device_id_type=MESH)

    def to(src, dst, ssem, rsem, pgroup, z=None):
        return pltpu.make_async_remote_copy(
            src_ref=src, dst_ref=dst, send_sem=ssem, recv_sem=rsem,
            device_id={"pgroup": pgroup, "tile": tile if z is None else z}, device_id_type=MESH,
        )

    edge = jnp.zeros((STRIPS, 8, 128), jnp.float32)
    for p in range(2):
        for b in range(2):
            for q in range(2):
                cols[p, b, q, :, pl.ds(0, 8), :] = edge
                cols[p, b, q, :, pl.ds(136, 8), :] = edge
    for p in range(4):
        for h in range(PARTS):
            ra[h][p, STRIPS] = jnp.zeros((ROWS, 128), jnp.float32)
            rb[h][p, STRIPS] = jnp.zeros((ROWS, 128), jnp.float32)
        rc[p, STRIPS] = jnp.zeros((8, 128), jnp.float32)

    @pl.when(tile == 0)
    def _():
        hin[...] = jnp.zeros(hin.shape, jnp.float32)

    params = [
        to(row_block, their_row, par_send.at[0], par_recv.at[0], partner),
        to(col_block, their_col, par_send.at[1], par_recv.at[1], partner),
    ]
    first = lax.broadcasted_iota(jnp.int32, (8, 128), 1) == 0

    def band_columns(p, b, h):
        g = col_frac[p]
        load_wait(p, b, h)
        low, high = extent(h)
        for r in range(low, high, 8):
            rows = pl.ds(128 * b + r, 8)
            before = [jnp.zeros((8, 128), jnp.float32)] * 2
            for k in range(STRIPS):
                lanes = pl.ds(128 * k, 128)
                beam = inp[p, 1, rows, lanes]
                for q in range(2):
                    value = beam * inp[p, core if q == 0 else 1 - core, rows, lanes]
                    rolled = pltpu.roll(value, 1, 1)
                    moved = jnp.where(first, before[q], rolled)
                    before[q] = rolled
                    cols[p, b, q, k, pl.ds(r + 8, 8), :] = (1.0 - g) * value + g * moved

    def mix(p, b, q, k, start, length):
        f = row_frac[p]
        s = band[p, b]
        near = cols[p, b, q, k, pl.ds(start + 8 - s, length), :]
        far = cols[p, b, q, k, pl.ds(start + 7 - s, length), :]
        return (1.0 - f) * near + f * far

    def band_rows_a(p, h):
        def step(k, carry):
            ta[p, h, k] = mix(p, 0, 1, k, h * ROWS, ROWS)
            ra[h][p, k] = mix(p, 0, 0, k, h * ROWS, ROWS)
            return carry

        lax.fori_loop(0, STRIPS, step, 0)

    def band_rows_b(p, h):
        def step(k, carry):
            for q in (1, 0):
                part = mix(p, 1, q, k, h * ROWS, ROWS)
                spot = tb.at[p, h, k] if q else rb[h].at[p, k]
                if h == 0:
                    spot[pl.ds(0, 8), :] = part[0:8] + mix(p, 0, q, k, 128, 8)
                    spot[pl.ds(8, ROWS - 8), :] = part[8:ROWS]
                    low = tc if q else rc
                    low[p, k] = mix(p, 1, q, k, 128, 8)
                else:
                    spot[...] = part
            return carry

        lax.fori_loop(0, STRIPS, step, 0)

    def strips(p, n):
        kind, h = divmod(n, PARTS)
        mine = (ta.at[p, h], tb.at[p, h], tc.at[p])[kind]
        theirs = (ra[h], rb[h], rc)[kind]
        return to(mine, theirs.at[2 + p, pl.ds(0, STRIPS)], strip_send.at[n], strip_recv.at[n], partner)

    def strips_both(n):
        kind, h = divmod(n, PARTS)
        mine = (ta.at[:, h], tb.at[:, h], tc)[kind]
        theirs = (ra[h], rb[h], rc)[kind]
        return to(mine, theirs.at[pl.ds(2, 2), pl.ds(0, STRIPS)], strip_send.at[n], strip_recv.at[n], partner)

    for copy in scalars:
        copy.wait()
    for p in range(2):
        band_columns(p, 0, top)
        if p == 0:
            load_all(top, 1)
            for h in reversed(range(top)):
                load_all(h, 0)
                load_all(h, 1)
        band_rows_a(p, top)

    pl.semaphore_wait(barrier, 9 + jnp.where(tile < 7, 1, 0) + jnp.where(tile > 0, 1, 0))
    for copy in params:
        copy.start()
    for p in range(2):
        strips(p, top).start()
    for p in range(2):
        band_columns(p, 1, top)
        band_rows_b(p, top)
        strips(p, PARTS + top).start()

    for copy in params:
        copy.wait()
    offs = [row_block[p] - 4 * tile for p in range(2)] + [their_row[p] - 4 * tile for p in range(2)]
    shifts = [col_block[p] for p in range(2)] + [their_col[p] for p in range(2)]

    def column_of(rel, c):
        return lax.rem(u + rel, 4) * su + lax.rem(v + lax.div(c, 2), 4) * sv + lax.rem(c, 2)

    def block_of(k):
        return lax.rem(k + lax.div(k, CHUNKS - 4), 4)

    def generate(k, block, rel, h, early=False):
        reach = [
            [jnp.where(block == offs[p] + n, STRIPS, 0) for n in range(3)] for p in range(4)
        ]

        def pick(k_in, limit):
            return jnp.where((k_in >= 0) & (k_in < limit), k_in, STRIPS)

        def step(c, carry):
            for half in range(UNROLL):
                spot = UNROLL * c + half
                j = column_of(rel, spot)
                total = None
                extra = None
                for p in range(4):
                    k_in = j - shifts[p]
                    part = ra[h][p, pick(k_in, reach[p][0])]
                    total = part if total is None else total + part
                    if not early:
                        total = total + rb[h][p, pick(k_in, reach[p][1])]
                    if h == 0:
                        tail = rc[p, pick(k_in, reach[p][2])]
                        extra = tail if extra is None else extra + tail
                if h == 0:
                    canvas[rel, k, spot, pl.ds(0, 8), :] = total[0:8] + extra
                    canvas[rel, k, spot, pl.ds(8, ROWS - 8), :] = total[8:ROWS]
                else:
                    canvas[rel, k, spot] = total
            return carry

        lax.fori_loop(0, 8 // UNROLL, step, 0)

        if h == 0:
            @pl.when(k == LAST)
            def _():
                canvas[rel, k, :, pl.ds(0, 8), :] = canvas[rel, k, :, pl.ds(0, 8), :] + hin[rel]

    def canvas_parts(k, rels):
        for h in range(PARTS):
            @pl.when(lax.div(k, 4) == PARTS - 1 - h)
            def _():
                for rel in rels:
                    generate(k, block_of(k), rel, h)

    def sent(stage, k):
        return send_sem.at[sum(SEND_SLOTS[:stage]) + lax.rem(k, SEND_SLOTS[stage])]

    def landed(stage, k):
        return recv_sem.at[sum(RECV_SLOTS[:stage]) + lax.rem(k, RECV_SLOTS[stage])]

    def copy_a(k, d):
        return to(canvas.at[2, k, pl.ds(4 * d, 4)], got_a.at[k, d], sent(0, k), landed(0, k), (up, um)[d])

    def copy_b(k, d):
        return to(canvas.at[1 + 2 * d, k], got_b.at[k, d], sent(1, k), landed(1, k), (up, um)[d])

    def copy_c(k, d):
        return to(canvas.at[0, k, 4 + d], got_c.at[k, d], sent(2, k), landed(2, k), (vp, vm)[d])

    def copy_d(k, d, half):
        other = (vp, vm)[d] - core + half
        return to(canvas.at[0, k, 2 + 4 * d + half], got_d.at[k, 2 * core + d], sent(3, k), last_recv.at[k], other)

    def copy_e(k):
        return to(canvas.at[0, k, 1 - core], got_d.at[k, 4], sent(2, k), last_recv.at[k], partner)

    def await_recv(stage, k):
        if stage >= 3:
            got = got_d.at[k, pl.ds(0, 5 if stage == 3 else 7)]
            to(got, got, end_send, last_recv.at[k], partner).wait_recv()
        else:
            got = (got_a, got_b, got_c)[stage].at[k]
            to(got, got, end_send, landed(stage, k), partner).wait_recv()

    def await_send(stage, k):
        size = (got_a.at[k], got_b.at[k], got_d.at[k, pl.ds(0, 3)], got_d.at[k, pl.ds(0, 4)])[stage]
        to(size, size, sent(stage, k), last_recv.at[0], partner).wait_send()

    def free(stage, k):
        @pl.when(k >= SEND_SLOTS[stage])
        def _():
            await_send(stage, k - SEND_SLOTS[stage])

    def stage_a(k):
        free(0, k)
        canvas_parts(k, (2,))
        copy_a(k, 0).start()
        copy_a(k, 1).start()

    def stage_b(k):
        @pl.when(k > 0)
        def _():
            canvas_parts(k, (1, 3, 0))

        await_recv(0, k)
        free(1, k)
        for d in range(2):
            part = pl.ds(4 * d, 4)
            canvas[1 + 2 * d, k, part] = canvas[1 + 2 * d, k, part] + got_a[k, d]
            copy_b(k, d).start()

    def stage_c(k):
        await_recv(1, k)
        free(2, k)
        for first_part, size in ((4, 2), (0, 4), (6, 2)):
            part = pl.ds(first_part, size)
            canvas[0, k, part] = canvas[0, k, part] + (got_b[k, 0, part] + got_b[k, 1, part])
            if first_part == 4:
                copy_c(k, 0).start()
                copy_c(k, 1).start()
        copy_e(k).start()

    def stage_d(k):
        await_recv(2, k)
        free(3, k)
        for d in range(2):
            spot = 2 + 5 * d
            canvas[0, k, spot] = canvas[0, k, spot] + got_c[k, d]
            copy_d(k, d, 0).start()
            copy_d(k, d, 1).start()

    def copy_end(n, half):
        other = (vp, vm, vq)[n] - core + half
        piece = canvas.at[0, LAST, (2, 6, 4)[n] + half]
        return to(piece, got_d.at[LAST, (2 * core, 2 * core + 1, 5 + core)[n]], end_send, last_recv.at[LAST], other)

    def copy_end_own():
        return to(canvas.at[0, LAST, 1 - core], got_d.at[LAST, 4], end_send, last_recv.at[LAST], partner)

    def stage_end():
        await_recv(1, LAST)
        for n, first_part in ((2, 4), (0, 2), (1, 6)):
            part = pl.ds(first_part, 2)
            canvas[0, LAST, part] = canvas[0, LAST, part] + (got_b[LAST, 0, part] + got_b[LAST, 1, part])
            for half in range(2):
                copy_end(n, half).start()
        part = pl.ds(0, 2)
        canvas[0, LAST, part] = canvas[0, LAST, part] + (got_b[LAST, 0, part] + got_b[LAST, 1, part])
        copy_end_own().start()

    def stage_f(k, last=False):
        await_recv(4 if last else 3, k)
        first_row = 128 * block_of(k) + ROWS * (PARTS - 1 - lax.div(k, 4))
        rows = pl.ds(pl.multiple_of(first_row, ROWS), ROWS)
        own = canvas[0, k, core] + (got_d[k, 2 * core] + got_d[k, 2 * core + 1])
        got = got_d[k, 4] + (got_d[k, 2 - 2 * core] + got_d[k, 3 - 2 * core])
        if last:
            own = own + got_d[k, 5 + core]
            got = got + got_d[k, 6 - core]
        above = jnp.where(core == 0, own, got)
        below = jnp.where(core == 0, got, own)
        numer[rows, :] = above
        weight[rows, :] = below
        normalised[rows, :] = above / jnp.maximum(below, 0.05)

    halo = to(hal, hin, hal_send, hal_recv, me, lax.rem(tile + 1, 8))

    def rest(h, p):
        band_columns(p, 0, h)
        band_rows_a(p, h)
        strips(p, h).start()
        band_columns(p, 1, h)
        band_rows_b(p, h)
        strips(p, PARTS + h).start()
        if h == 0:
            strips(p, 2 * PARTS).start()

    def rest_wait(h):
        strips_both(h).wait_recv()
        strips_both(PARTS + h).wait_recv()
        if h == 0:
            strips_both(2 * PARTS).wait_recv()

    def send_halo():
        def step(n, carry):
            j = column_of(lax.div(n, 8), lax.rem(n, 8))
            total = None
            for p in range(4):
                k_in = j - shifts[p]
                ic = jnp.where((k_in >= 0) & (k_in < STRIPS) & (offs[p] == 2), k_in, STRIPS)
                tail = rc[p, ic]
                total = tail if total is None else total + tail
            hal[lax.div(n, 8), lax.rem(n, 8)] = total
            return carry

        lax.fori_loop(0, 32, step, 0)
        halo.start()

    def iteration(i, carry):
        for h in reversed(range(PARTS - 1)):
            @pl.when(i == part_start(h))
            def _():
                rest_wait(h)

        @pl.when((i == LAST) & (tile > 0))
        def _():
            halo.wait_recv()

        @pl.when(i < CHUNKS)
        def _():
            stage_a(i)

        for h in reversed(range(PARTS - 1)):
            for p in range(2):
                if rest_step(h, p) >= LAG_B:
                    @pl.when(i == rest_step(h, p))
                    def _():
                        rest(h, p)

        stages = ((LAG_B, stage_b, CHUNKS), (LAG_D, stage_d, LAST), (LAG_F, stage_f, LAST), (LAG_C, stage_c, LAST))
        for lag, stage, count in stages:
            @pl.when((i >= lag) & (i < count + lag))
            def _():
                stage(i - lag)

        @pl.when(i == LAST + LAG_C)
        def _():
            stage_end()

        @pl.when((i == part_start(0)) & (tile < 7))
        def _():
            send_halo()

        return carry

    def part_start(h):
        return 4 * (PARTS - 1 - h)

    def rest_step(h, p):
        return part_start(h) - (2 if h == top - 1 else 3) + p

    strips_both(top).wait_recv()
    generate(0, 0, 2, top, True)
    copy_a(0, 0).start()
    copy_a(0, 1).start()
    for rel in (1, 3, 0):
        generate(0, 0, rel, top, True)
    strips_both(PARTS + top).wait_recv()
    for i in range(1, LAG_B):
        generate(i, i, 2, top)
        copy_a(i, 0).start()
        copy_a(i, 1).start()
        for p in range(2):
            if i == rest_step(top - 1, p):
                rest(top - 1, p)
    lax.fori_loop(LAG_B, LAST + LAG_F, iteration, 0)
    stage_f(LAST, True)

    for stage in range(4):
        count = CHUNKS if stage < 2 else LAST
        for k in range(count - SEND_SLOTS[stage], count):
            await_send(stage, k)
    to(got_d.at[LAST], got_d.at[LAST], end_send, last_recv.at[0], partner).wait_send()
    for n in range(2 * PARTS + 1):
        strips_both(n).wait_send()

    @pl.when(tile < 7)
    def _():
        halo.wait_send()


def store(numer, weight, normalised, numer_out, weight_out, normalised_out, sem):
    pairs = ((numer, numer_out), (weight, weight_out), (normalised, normalised_out))
    copies = [pltpu.make_async_copy(a, b, sem.at[n]) for n, (a, b) in enumerate(pairs)]
    for copy in copies:
        copy.start()
    for copy in copies:
        copy.wait()


def body(images, beams, row_block, col_block, band, row_frac, col_frac):
    f32 = jnp.float32
    vmem = lambda *shape: pltpu.VMEM(shape, f32)
    dma = pltpu.SemaphoreType.DMA
    piece = jax.ShapeDtypeStruct((SKY, 128), f32)
    hbm = pl.BlockSpec(memory_space=pl.ANY)
    local = pl.BlockSpec(memory_space=pltpu.VMEM)
    found = pl.pallas_call(
        kernel,
        out_shape=(pltpu.VMEM((SKY, 128), f32),) * 3,
        in_specs=[hbm] * 7,
        out_specs=(local, local, local),
        scratch_shapes=[
            vmem(2, 2, 256, 2048),
            vmem(2, 2, 2, STRIPS, 144, 128),
            [vmem(4, STRIPS + 1, ROWS, 128) for _ in range(PARTS)],
            [vmem(4, STRIPS + 1, ROWS, 128) for _ in range(PARTS)],
            vmem(4, STRIPS + 1, 8, 128),
            vmem(2, PARTS, STRIPS, ROWS, 128),
            vmem(2, PARTS, STRIPS, ROWS, 128),
            vmem(2, STRIPS, 8, 128),
            vmem(4, CHUNKS, 8, ROWS, 128),
            vmem(4, 8, 8, 128),
            vmem(4, 8, 8, 128),
            vmem(CHUNKS, 2, 4, ROWS, 128),
            vmem(CHUNKS, 2, 8, ROWS, 128),
            vmem(CHUNKS, 2, ROWS, 128),
            vmem(CHUNKS, 7, ROWS, 128),
            pltpu.SMEM((2,), jnp.int32),
            pltpu.SMEM((2,), jnp.int32),
            pltpu.SMEM((2, 2), jnp.int32),
            pltpu.SMEM((2,), f32),
            pltpu.SMEM((2,), f32),
            pltpu.SMEM((2,), jnp.int32),
            pltpu.SMEM((2,), jnp.int32),
            dma((2 * PARTS + 1,)),
            dma((5,)),
            dma((2,)),
            dma((2,)),
            dma((2 * PARTS + 1,)),
            dma((2 * PARTS + 1,)),
            dma,
            dma,
            dma((sum(SEND_SLOTS),)),
            dma((sum(RECV_SLOTS),)),
            dma((CHUNKS,)),
            dma,
        ],
        compiler_params=pltpu.CompilerParams(
            collective_id=0, has_side_effects=True, vmem_limit_bytes=60_000_000
        ),
    )(images, beams, row_block, col_block, band, row_frac, col_frac)
    return pl.pallas_call(
        store,
        out_shape=(piece, piece, piece),
        in_specs=[local, local, local],
        out_specs=(hbm, hbm, hbm),
        scratch_shapes=[dma((3,))],
    )(*[pltpu.with_memory_space_constraint(a, pltpu.VMEM) for a in found])


def solution(mesh):
    return jax.shard_map(
        body,
        mesh=mesh,
        in_specs=(
            P(("pgroup", "tile"), None, None),
            P(("pgroup", "tile"), None, None),
            P(("pgroup", "tile")),
            P(("pgroup", "tile")),
            P(("pgroup", "tile"), None),
            P(("pgroup", "tile")),
            P(("pgroup", "tile")),
        ),
        out_specs=(P("tile", "pgroup"), P("tile", "pgroup"), P("tile", "pgroup")),
        check_vma=False,
    )
```
